256 devices in a mesh: rows: 32 (over z, y), tp: 4 (over x), unit: 2 (over core).
Axes of the slice: x: 4, y: 4, z: 8, core: 2. Of those that a mesh axis runs over, the one named last changes fastest.
Arguments:
- w_query: bfloat16 [5120, 4096], P(('unit', 'rows'), 'tp'), parts along dimension 0, may hold values from -0.125 to 0.125
- low_query: bfloat16 [5120, 64], P(('unit', 'rows')), parts along dimension 0, may hold values from -0.125 to 0.125
- high_query: bfloat16 [128, 4096], P('unit', 'tp'), parts along dimension 0, may hold values from -0.75 to 0.75
- w_key: bfloat16 [5120, 1024], P(('unit', 'rows'), 'tp'), parts along dimension 0, may hold values from -0.125 to 0.125
- low_key: bfloat16 [5120, 64], P(('unit', 'rows')), parts along dimension 0, may hold values from -0.125 to 0.125
- high_key: bfloat16 [128, 1024], P('unit', 'tp'), parts along dimension 0, may hold values from -0.75 to 0.75
- w_value: bfloat16 [5120, 1024], P(('unit', 'rows'), 'tp'), parts along dimension 0, may hold values from -0.125 to 0.125
- low_value: bfloat16 [5120, 64], P(('unit', 'rows')), parts along dimension 0, may hold values from -0.125 to 0.125
- high_value: bfloat16 [128, 1024], P('unit', 'tp'), parts along dimension 0, may hold values from -0.75 to 0.75
- w_mixed: bfloat16 [8192, 2560], P(('unit', 'tp'), 'rows'), parts along dimension 0, may hold values from -0.09375 to 0.09375
- low_mixed: bfloat16 [8192, 64], P(('unit', 'tp')), parts along dimension 0, may hold values from -0.09375 to 0.09375
- high_mixed: bfloat16 [128, 2560], P('unit', 'rows'), parts along dimension 0, may hold values from -0.75 to 0.75
- norm_train: float32 [5120], P(('unit', 'rows', 'tp')), parts along dimension 0, may hold values from 0.25 to 1.75
- norm_step: float32 [5120], P(('unit', 'rows', 'tp')), parts along dimension 0, may hold values from -0.3 to 0.3
Outputs:
- final_query: bfloat16 [5120, 4096], P('unit', 'tp'), parts along dimension 0
- final_key: bfloat16 [5120, 1024], P('unit', 'tp'), parts along dimension 0
- final_value: bfloat16 [5120, 1024], P('unit', 'tp'), parts along dimension 0
- final_mixed: bfloat16 [8192, 2560], P(('unit', 'tp')), parts along dimension 0
- serve_norm: bfloat16 [5120], P('unit'), parts along dimension 0
The draws below stay inside these ranges and needn't reach their ends.
There are 2 independent parts, one for each index of `unit`. The reference program is written for one: setup_inputs(seed, part) draws one part's arguments, and reference() takes and returns one part's arrays. A program takes and returns all parts, laid end to end along the dimension named above; each array names one. Nothing has to cross between parts.
All inputs are finite; a program needn't handle non-finite values.
Results may differ from the reference program's by a relative error of at most 0.001.
Values may be sent and summed in bfloat16 or wider, within the bound.
A program may use at most 128 MiB of HBM per device.

```python
import jax
import jax.numpy as jnp

D_MODEL = 2560
Q_DIM = 4096
KV_DIM = 1024
RANK = 64


def block_levels(own_key, dims, pieces, smallest, largest):
    gain, own = 1.0, jax.random.fold_in(own_key, 6)
    for position, parts in pieces:
        steps = jnp.exp(jax.random.uniform(jax.random.fold_in(own, position), (parts,), jnp.float32, smallest / len(pieces), largest / len(pieces)))
        gain = gain * jnp.repeat(steps, dims[position] // parts).reshape([-1 if axis == position else 1 for axis in range(len(dims))])
    return gain


def gaussian(stream_key, shape, deviation, limit, pieces=(), dtype=jnp.bfloat16):
    drawn = jax.random.normal(stream_key, shape, jnp.float32) * deviation
    if len(pieces) > 0:
        drawn = block_levels(stream_key, shape, pieces, -0.22, 0.18) * drawn
    return jnp.clip(drawn, min=-limit, max=limit).astype(dtype)


def setup_inputs(seed: int = 0, part: int = 0) -> dict:
    key_of = jax.random.split(jax.random.key(seed), 15)
    own_keys = jax.random.split(jax.random.fold_in(key_of[14], part), 15)
    return {
        "w_query": gaussian(own_keys[0], (D_MODEL, Q_DIM), D_MODEL ** -0.5, 0.125, ((0, 32), (1, 4))),
        "low_query": gaussian(own_keys[1], (D_MODEL, RANK), D_MODEL ** -0.5, 0.125, ((0, 32),)),
        "high_query": gaussian(own_keys[2], (RANK, Q_DIM), RANK ** -0.5, 0.75, ((1, 4),)),
        "w_key": gaussian(own_keys[3], (D_MODEL, KV_DIM), D_MODEL ** -0.5, 0.125, ((0, 32), (1, 4))),
        "low_key": gaussian(own_keys[4], (D_MODEL, RANK), D_MODEL ** -0.5, 0.125, ((0, 32),)),
        "high_key": gaussian(own_keys[5], (RANK, KV_DIM), RANK ** -0.5, 0.75, ((1, 4),)),
        "w_value": gaussian(own_keys[6], (D_MODEL, KV_DIM), D_MODEL ** -0.5, 0.125, ((0, 32), (1, 4))),
        "low_value": gaussian(own_keys[7], (D_MODEL, RANK), D_MODEL ** -0.5, 0.125, ((0, 32),)),
        "high_value": gaussian(own_keys[8], (RANK, KV_DIM), RANK ** -0.5, 0.75, ((1, 4),)),
        "w_mixed": gaussian(own_keys[9], (Q_DIM, D_MODEL), Q_DIM ** -0.5, 0.09375, ((0, 4), (1, 32))),
        "low_mixed": gaussian(own_keys[10], (Q_DIM, RANK), Q_DIM ** -0.5, 0.09375, ((0, 4),)),
        "high_mixed": gaussian(own_keys[11], (RANK, D_MODEL), RANK ** -0.5, 0.75, ((1, 32),)),
        "norm_train": jnp.clip(1.0 + 0.15 * jax.random.normal(own_keys[12], (D_MODEL,), jnp.float32), 0.25, 1.75),
        "norm_step": jnp.clip(jax.random.uniform(own_keys[13], (D_MODEL,), jnp.float32, -0.3, 0.3) * block_levels(own_keys[13], (D_MODEL,), ((0, 128),), -0.4, 0.0), -0.3, 0.3),
    }


mix_rate = 0.5


def reference(w_query, low_query, high_query, w_key, low_key, high_key, w_value, low_value, high_value, w_mixed, low_mixed, high_mixed, norm_train, norm_step):
    result_query = w_query.astype(jnp.float32) + mix_rate * jnp.dot(low_query, high_query, preferred_element_type=jnp.float32)
    result_key = w_key.astype(jnp.float32) + mix_rate * jnp.dot(low_key, high_key, preferred_element_type=jnp.float32)
    result_value = w_value.astype(jnp.float32) + mix_rate * jnp.dot(low_value, high_value, preferred_element_type=jnp.float32)
    result_mixed = w_mixed.astype(jnp.float32) + mix_rate * jnp.dot(low_mixed, high_mixed, preferred_element_type=jnp.float32)
    final_query = result_query.astype(jnp.bfloat16)
    final_key = result_key.astype(jnp.bfloat16)
    final_value = result_value.astype(jnp.bfloat16)
    final_mixed = result_mixed.astype(jnp.bfloat16)
    serve_norm = (norm_train + norm_step).astype(jnp.bfloat16)
    return final_query, final_key, final_value, final_mixed, serve_norm
```

```python
import functools
import heapq

import jax
import jax.numpy as jnp
from jax import lax
from jax.experimental import pallas as pl
from jax.experimental.pallas import tpu as pltpu
from jax.sharding import PartitionSpec as P

MESH = pl.DeviceIdType.MESH
UNIT_ROWS = ("unit", "rows")
UNIT_ROWS_TP = ("unit", "rows", "tp")

mix_rate = 0.5

NY, NZ = 4, 8
SIZE = {"y": NY, "z": NZ}
LINKS = (("y", 1), ("y", -1), ("z", 1), ("z", -1))
RATE, LATENCY, LEAD = 46.6e3, 2.0, 3.0


def reach(n, step, side):
    return n // 2 if (side == 0) == (step > 0) else n - 1 - n // 2


def onward(piece, via, hops):
    first, second = ("y", "z") if piece["y_first"] else ("z", "y")
    if via is None:
        out = [((axis, step), 1) for axis in (first, second) for step in (1, -1)]
    else:
        out = [(via, hops + 1)]
        if via[0] == first:
            out += [((second, step), 1) for step in (1, -1)]
    return [(l, h) for l, h in out if h <= reach(SIZE[l[0]], l[1], piece["side"])]


def plan(pieces):
    def urgency(piece, link, hops):
        left = reach(SIZE[link[0]], link[1], piece["side"]) - hops
        first, second = ("y", "z") if piece["y_first"] else ("z", "y")
        return piece["phase"], -(left + (SIZE[second] // 2 if link[0] == first else 0))

    queue, free, seq = {l: [] for l in LINKS}, dict.fromkeys(LINKS, 0.0), 0
    events, steps, got, last = [], [], {}, dict.fromkeys(LINKS, 0.0)

    def hold(k, origin, via, hops):
        nonlocal seq
        for link, h in onward(pieces[k], via, hops):
            seq += 1
            heapq.heappush(queue[link], (urgency(pieces[k], link, h), seq, k, origin, h))

    for k in range(len(pieces)):
        got[k, (0, 0)] = 0.0
        hold(k, (0, 0), None, 0)
    now = 0.0
    while True:
        for link in LINKS:
            if free[link] <= now + 1e-9 and queue[link]:
                _, _, k, origin, h = heapq.heappop(queue[link])
                issue = max(got[k, origin], now - LEAD, last[link])
                last[link] = issue
                seq += 1
                steps.append((issue, seq, "send", k, origin, link))
                free[link] = now + pieces[k]["bytes"] / RATE
                dy, dz = origin
                there = ((dy - link[1]) % NY, dz) if link[0] == "y" else (dy, (dz - link[1]) % NZ)
                heapq.heappush(events, (free[link], seq, None))
                heapq.heappush(events, (free[link] + LATENCY, seq, (k, there, link, h)))
        if not events:
            break
        now = events[0][0]
        while events and events[0][0] <= now + 1e-9:
            _, _, landed = heapq.heappop(events)
            if landed is not None:
                k, origin, link, h = landed
                got[k, origin] = now
                seq += 1
                steps.append((now, seq, "wait", k, origin, link))
                hold(k, origin, link, h)
    steps.sort(key=lambda s: (s[0], s[2] == "send", s[1]))
    return [(t, *rest) for t, _, *rest in steps]


def make_pieces(depth, mixed, rest):
    pieces = []
    for phase, buffer, columns in ((0, "mixed", mixed), (1, "rest", rest)):
        cut = depth * 2 // 5 // 16 * 16
        for y_first, low, count in ((True, 0, cut), (False, cut, depth - cut)):
            for side in (0, 1):
                pieces.append(
                    dict(
                        phase=phase,
                        buffer=buffer,
                        y_first=y_first,
                        side=side,
                        row=low,
                        rows=count,
                        col=side * columns // 2,
                        cols=columns // 2,
                        bytes=count * columns,
                    )
                )
    return pieces


def merged(w, low_t, high):
    product = lax.dot_general(
        low_t, high, (((0,), (0,)), ((), ())), preferred_element_type=jnp.float32
    )
    return (w.astype(jnp.float32) + mix_rate * product).astype(jnp.bfloat16)


def gather_kernel(
    n_tp,
    depth,
    w_query,
    low_query,
    high_query,
    w_key,
    low_key,
    high_key,
    w_value,
    low_value,
    high_value,
    w_mixed,
    low_mixed,
    high_mixed,
    norm_train,
    norm_step,
    rest,
    mixed_out,
    norm_out,
    mixed,
    peers,
    norms,
    sent,
    got,
    sent_norm,
    got_norm,
):
    rows, t = lax.axis_index("rows"), lax.axis_index("tp")
    z, y = rows // NY, lax.rem(rows, NY)
    ys = [lax.rem(y + d, NY) for d in range(NY)]
    zs = [lax.rem(z + d, NZ) for d in range(NZ)]
    ts = [lax.rem(t + d, n_tp) for d in range(n_tp)]
    at = {(dy, dz): zs[dz] * NY + ys[dy] for dy in range(NY) for dz in range(NZ)}
    to = {
        ("y", 1): at[1, 0],
        ("y", -1): at[NY - 1, 0],
        ("z", 1): at[0, 1],
        ("z", -1): at[0, NZ - 1],
    }

    barrier = pltpu.get_barrier_semaphore()
    for link in LINKS:
        pl.semaphore_signal(barrier, 1, device_id={"rows": to[link]}, device_id_type=MESH)
    for d in range(1, n_tp):
        pl.semaphore_signal(barrier, 1, device_id={"tp": ts[d]}, device_id_type=MESH)

    mine = pl.ds(pl.multiple_of(rows * depth, 16), depth)
    q, k = w_query.shape[1], w_key.shape[1]
    mixed[mine, :] = merged(w_mixed[...], high_mixed[...], low_mixed[...])
    rest[mine, :q] = merged(w_query[...], low_query[...], high_query[...])
    rest[mine, q : q + k] = merged(w_key[...], low_key[...], high_key[...])
    rest[mine, q + k :] = merged(w_value[...], low_value[...], high_value[...])
    share = norm_train.shape[1]
    gain = norm_train[...] + norm_step[...]
    wide = jnp.concatenate([gain, jnp.zeros((1, 128 - share), jnp.float32)], axis=1)
    peers[t] = pltpu.roll(wide, t * share, 1)

    pl.semaphore_wait(barrier, len(LINKS) + n_tp - 1)

    buffers = {"mixed": mixed, "rest": rest}
    pieces = make_pieces(depth, mixed.shape[1], rest.shape[1])

    def copy(k, origin, link):
        p, r = pieces[k], at[origin]
        ref = buffers[p["buffer"]].at[
            pl.ds(pl.multiple_of(r * depth + p["row"], 16), p["rows"]),
            pl.ds(p["col"], p["cols"]),
        ]
        return pltpu.make_async_remote_copy(
            src_ref=ref,
            dst_ref=ref,
            send_sem=sent.at[p["phase"]],
            recv_sem=got.at[k, r],
            device_id={"rows": to[link]},
            device_id_type=MESH,
        )

    def norm_copy(ref, n, axis, index):
        return pltpu.make_async_remote_copy(
            src_ref=ref,
            dst_ref=ref,
            send_sem=sent_norm.at[n],
            recv_sem=got_norm.at[n],
            device_id={axis: index},
            device_id_type=MESH,
        )

    def peer_copy(d):
        return norm_copy(peers.at[t], d - 1, "tp", ts[d])

    def y_copy(n):
        dy, link = ((0, ("y", 1)), (0, ("y", -1)), (NY - 1, ("y", 1)))[n]
        return norm_copy(norms.at[pl.ds(at[dy, 0], 1)], 3 + n, "rows", to[link])

    def z_copy(n):
        dz, link = (-n % NZ, ("z", 1)) if n < 4 else (n - 4, ("z", -1))
        return norm_copy(norms.at[pl.ds(zs[dz] * NY, NY)], 6 + n, "rows", to[link])

    def norm_step_0():
        for d in range(1, n_tp):
            peer_copy(d).start()

    def norm_step_1():
        for d in range(1, n_tp):
            peer_copy(d).wait_recv()
        norms[rows] = sum(peers[d] for d in range(n_tp))

    def norm_step_2():
        y_copy(0).start()
        y_copy(1).start()

    def norm_step_3():
        y_copy(0).wait_recv()
        y_copy(2).start()
        y_copy(1).wait_recv()

    def norm_step_4():
        y_copy(2).wait_recv()
        z_copy(0).start()
        z_copy(4).start()

    def norm_hop(n):
        z_copy(n - 1).wait_recv()
        z_copy(n).start()
        if n < 3:
            z_copy(n + 3).wait_recv()
            z_copy(n + 4).start()

    def norm_last():
        z_copy(3).wait_recv()
        z_copy(6).wait_recv()
        n_norm = norms.shape[0] * share * n_tp
        lane = lax.broadcasted_iota(jnp.int32, (1, 128), 1)
        lines = [jnp.zeros((1, 128), jnp.float32) for _ in range(n_norm // 128)]
        width = share * n_tp
        for r in range(norms.shape[0]):
            line, off = divmod(r * width, 128)
            part = pltpu.roll(norms[r], off, 1) if off else norms[r]
            lines[line] += jnp.where(lane >= off, part, 0.0)
            if off + width > 128:
                lines[line + 1] += jnp.where(lane < off + width - 128, part, 0.0)
        norm_out[...] = jnp.concatenate(lines, axis=0).astype(norm_out.dtype)

    def turn(j):
        part = mixed[128 * j : 128 * (j + 1), :]
        mixed_out[:, 128 * j : 128 * (j + 1)] = part.T

    steps = plan(pieces)
    turned = [s[0] for s in steps if s[1] == "wait" and pieces[s[2]]["phase"] == 0][-1]
    end = steps[-1][0]
    n_turn = mixed.shape[0] // 128
    side_jobs = [(0.5, norm_step_0), (6.0, norm_step_1), (8.0, norm_step_2), (14.0, norm_step_3)]
    side_jobs += [(20.0, norm_step_4)]
    side_jobs += [(20.0 + 6.0 * n, functools.partial(norm_hop, n)) for n in range(1, 4)]
    side_jobs += [(46.0, norm_last)]
    gap = (end - 8.0 - turned) / n_turn
    side_jobs += [
        (turned + 0.01 + gap * j, functools.partial(turn, j)) for j in range(n_turn)
    ]
    side_jobs.sort(key=lambda job: job[0])

    for when, what, k, origin, link in steps:
        while side_jobs and side_jobs[0][0] < when:
            side_jobs.pop(0)[1]()
        if what == "wait":
            copy(k, origin, link).wait_recv()
        else:
            copy(k, origin, link).start()
    for _, job in side_jobs:
        job()

    n_rows = mixed.shape[0]
    for phase, buffer in ((0, mixed), (1, rest)):
        others = buffer.at[pl.ds(0, n_rows - depth)]
        pltpu.make_async_remote_copy(
            src_ref=others,
            dst_ref=others,
            send_sem=sent.at[phase],
            recv_sem=got.at[0, 0],
            device_id={"rows": to["y", 1]},
            device_id_type=MESH,
        ).wait_send()
    for d in range(1, n_tp):
        peer_copy(d).wait_send()
    for n in range(3):
        y_copy(n).wait_send()
    for n in range(7):
        z_copy(n).wait_send()


def put_kernel(rest, mixed, final_query, final_key, final_value, final_mixed, sems):
    q, k = final_query.shape[1], final_key.shape[1]
    copies = [
        pltpu.make_async_copy(mixed, final_mixed, sems.at[0]),
        pltpu.make_async_copy(rest.at[:, pl.ds(0, q)], final_query, sems.at[1]),
        pltpu.make_async_copy(rest.at[:, pl.ds(q, k)], final_key, sems.at[2]),
        pltpu.make_async_copy(rest.at[:, pl.ds(q + k, k)], final_value, sems.at[3]),
    ]
    for c in copies:
        c.start()
    for c in copies:
        c.wait()


def shards(n_rows, n_tp, *args):
    (
        w_query,
        low_query,
        high_query,
        w_key,
        low_key,
        high_key,
        w_value,
        low_value,
        high_value,
        w_mixed,
        low_mixed,
        high_mixed,
        norm_train,
        norm_step,
    ) = args
    depth, q, k = w_query.shape[0], w_query.shape[1], w_key.shape[1]
    m = w_mixed.shape[0]
    total = n_rows * depth
    n_norm = n_rows * n_tp * norm_train.shape[0]
    bf16, f32 = jnp.bfloat16, jnp.float32
    vmem = pl.BlockSpec(memory_space=pltpu.VMEM)
    n_pieces = len(make_pieces(depth, m, q + 2 * k))
    rest, mixed, norm = pl.pallas_call(
        functools.partial(gather_kernel, n_tp, depth),
        out_shape=(
            pltpu.VMEM((total, q + 2 * k), bf16),
            pltpu.VMEM((m, total), bf16),
            jax.ShapeDtypeStruct((n_norm // 128, 128), bf16),
        ),
        in_specs=[vmem] * 14,
        out_specs=(vmem, vmem, vmem),
        scratch_shapes=[
            pltpu.VMEM((total, m), bf16),
            pltpu.VMEM((n_tp, 1, 128), f32),
            pltpu.VMEM((n_rows, 1, 128), f32),
            pltpu.SemaphoreType.DMA((2,)),
            pltpu.SemaphoreType.DMA((n_pieces, n_rows)),
            pltpu.SemaphoreType.DMA((13,)),
            pltpu.SemaphoreType.DMA((13,)),
        ],
        compiler_params=pltpu.CompilerParams(
            collective_id=0, has_side_effects=True, vmem_limit_bytes=40 << 20
        ),
        name="gather",
    )(
        w_query,
        low_query.T,
        high_query,
        w_key,
        low_key.T,
        high_key,
        w_value,
        low_value.T,
        high_value,
        w_mixed.T,
        low_mixed.T,
        high_mixed,
        norm_train.reshape(1, -1),
        norm_step.reshape(1, -1),
    )
    hbm = pl.BlockSpec(memory_space=pltpu.HBM)
    final_query, final_key, final_value, final_mixed = pl.pallas_call(
        put_kernel,
        out_shape=(
            jax.ShapeDtypeStruct((total, q), bf16),
            jax.ShapeDtypeStruct((total, k), bf16),
            jax.ShapeDtypeStruct((total, k), bf16),
            jax.ShapeDtypeStruct((m, total), bf16),
        ),
        in_specs=[vmem] * 2,
        out_specs=(hbm,) * 4,
        scratch_shapes=[pltpu.SemaphoreType.DMA((4,))],
        name="put",
    )(rest, mixed)
    return final_query, final_key, final_value, final_mixed, norm.reshape(-1)


def solution(mesh):
    return jax.shard_map(
        functools.partial(shards, mesh.shape["rows"], mesh.shape["tp"]),
        mesh=mesh,
        in_specs=(
            P(UNIT_ROWS, "tp"),
            P(UNIT_ROWS, None),
            P("unit", "tp"),
            P(UNIT_ROWS, "tp"),
            P(UNIT_ROWS, None),
            P("unit", "tp"),
            P(UNIT_ROWS, "tp"),
            P(UNIT_ROWS, None),
            P("unit", "tp"),
            P(("unit", "tp"), "rows"),
            P(("unit", "tp"), None),
            P("unit", "rows"),
            P(UNIT_ROWS_TP),
            P(UNIT_ROWS_TP),
        ),
        out_specs=(
            P("unit", "tp"),
            P("unit", "tp"),
            P("unit", "tp"),
            P(("unit", "tp"), None),
            P("unit"),
        ),
        check_vma=False,
    )
```

```python
import functools
import heapq

import jax
import jax.numpy as jnp
from jax import lax
from jax.experimental import pallas as pl
from jax.experimental.pallas import tpu as pltpu
from jax.sharding import PartitionSpec as P

MESH = pl.DeviceIdType.MESH
UNIT_ROWS = ("unit", "rows")
UNIT_ROWS_TP = ("unit", "rows", "tp")

mix_rate = 0.5
N_ARGS = 14

NY, NZ = 4, 8
SIZE = {"y": NY, "z": NZ}
LINKS = (("y", 1), ("y", -1), ("z", 1), ("z", -1))
RATE, LATENCY, LEAD = 46.6e3, 2.0, 3.0


def reach(n, step, side):
    return n // 2 if (side == 0) == (step > 0) else n - 1 - n // 2


def onward(piece, via, hops):
    first, second = ("y", "z") if piece["y_first"] else ("z", "y")
    if via is None:
        out = [((axis, step), 1) for axis in (first, second) for step in (1, -1)]
    else:
        out = [(via, hops + 1)]
        if via[0] == first:
            out += [((second, step), 1) for step in (1, -1)]
    return [(l, h) for l, h in out if h <= reach(SIZE[l[0]], l[1], piece["side"])]


def plan(pieces):
    def urgency(piece, link, hops):
        left = reach(SIZE[link[0]], link[1], piece["side"]) - hops
        first, second = ("y", "z") if piece["y_first"] else ("z", "y")
        return piece["phase"], -(left + (SIZE[second] // 2 if link[0] == first else 0))

    queue, free, seq = {l: [] for l in LINKS}, dict.fromkeys(LINKS, 0.0), 0
    events, steps, got, last = [], [], {}, dict.fromkeys(LINKS, 0.0)

    def hold(k, origin, via, hops):
        nonlocal seq
        for link, h in onward(pieces[k], via, hops):
            seq += 1
            heapq.heappush(queue[link], (urgency(pieces[k], link, h), seq, k, origin, h))

    for k in range(len(pieces)):
        got[k, (0, 0)] = 0.0
        hold(k, (0, 0), None, 0)
    now = 0.0
    while True:
        for link in LINKS:
            if free[link] <= now + 1e-9 and queue[link]:
                _, _, k, origin, h = heapq.heappop(queue[link])
                issue = max(got[k, origin], now - LEAD, last[link])
                last[link] = issue
                seq += 1
                steps.append((issue, seq, "send", k, origin, link))
                free[link] = now + pieces[k]["bytes"] / RATE
                dy, dz = origin
                there = ((dy - link[1]) % NY, dz) if link[0] == "y" else (dy, (dz - link[1]) % NZ)
                heapq.heappush(events, (free[link], seq, None))
                heapq.heappush(events, (free[link] + LATENCY, seq, (k, there, link, h)))
        if not events:
            break
        now = events[0][0]
        while events and events[0][0] <= now + 1e-9:
            _, _, landed = heapq.heappop(events)
            if landed is not None:
                k, origin, link, h = landed
                got[k, origin] = now
                seq += 1
                steps.append((now, seq, "wait", k, origin, link))
                hold(k, origin, link, h)
    steps.sort(key=lambda s: (s[0], s[2] == "send", s[1]))
    return [(t, *rest) for t, _, *rest in steps]


def make_pieces(depth, mixed, rest):
    pieces = []
    for phase, buffer, columns in ((0, "mixed", mixed), (1, "rest", rest)):
        cut = depth * 2 // 5 // 16 * 16
        for y_first, low, count in ((True, 0, cut), (False, cut, depth - cut)):
            for side in (0, 1):
                pieces.append(
                    dict(
                        phase=phase,
                        buffer=buffer,
                        y_first=y_first,
                        side=side,
                        row=low,
                        rows=count,
                        col=side * columns // 2,
                        cols=columns // 2,
                        bytes=count * columns,
                    )
                )
    return pieces


def merged(w, low_t, high):
    product = lax.dot_general(
        low_t, high, (((0,), (0,)), ((), ())), preferred_element_type=jnp.float32
    )
    return (w.astype(jnp.float32) + mix_rate * product).astype(jnp.bfloat16)


def gather_kernel(n_tp, depth, *refs):
    given, (rest, mixed_out, norm_out), held = refs[:N_ARGS], refs[N_ARGS : N_ARGS + 3], refs[N_ARGS + 3 :]
    fetched, (mixed, peers, norms, fetch_sem, sent, got, sent_norm, got_norm) = (
        held[:N_ARGS],
        held[N_ARGS:],
    )
    w_query, low_query, high_query, w_key, low_key, high_key, w_value, low_value, high_value = fetched[:9]
    w_mixed, low_mixed, high_mixed, norm_train, norm_step = fetched[9:]
    fetches = [
        pltpu.make_async_copy(a, b, fetch_sem.at[n])
        for n, (a, b) in enumerate(zip(given, fetched))
    ]
    for n in (*range(9, N_ARGS), *range(9)):
        fetches[n].start()

    rows, t = lax.axis_index("rows"), lax.axis_index("tp")
    z, y = rows // NY, lax.rem(rows, NY)
    ys = [lax.rem(y + d, NY) for d in range(NY)]
    zs = [lax.rem(z + d, NZ) for d in range(NZ)]
    ts = [lax.rem(t + d, n_tp) for d in range(n_tp)]
    at = {(dy, dz): zs[dz] * NY + ys[dy] for dy in range(NY) for dz in range(NZ)}
    to = {
        ("y", 1): at[1, 0],
        ("y", -1): at[NY - 1, 0],
        ("z", 1): at[0, 1],
        ("z", -1): at[0, NZ - 1],
    }

    barrier = pltpu.get_barrier_semaphore()
    for link in LINKS:
        pl.semaphore_signal(barrier, 1, device_id={"rows": to[link]}, device_id_type=MESH)
    for d in range(1, n_tp):
        pl.semaphore_signal(barrier, 1, device_id={"tp": ts[d]}, device_id_type=MESH)

    mine = pl.ds(pl.multiple_of(rows * depth, 16), depth)
    q, k = w_query.shape[1], w_key.shape[1]
    for n in range(9, N_ARGS):
        fetches[n].wait()
    mixed[mine, :] = merged(w_mixed[...], high_mixed[...], low_mixed[...])
    share = norm_train.shape[1]
    gain = norm_train[...] + norm_step[...]
    wide = jnp.concatenate([gain, jnp.zeros((1, 128 - share), jnp.float32)], axis=1)
    peers[t] = pltpu.roll(wide, t * share, 1)

    def merge_rest():
        for n in range(9):
            fetches[n].wait()
        rest[mine, :q] = merged(w_query[...], low_query[...], high_query[...])
        rest[mine, q : q + k] = merged(w_key[...], low_key[...], high_key[...])
        rest[mine, q + k :] = merged(w_value[...], low_value[...], high_value[...])

    pl.semaphore_wait(barrier, len(LINKS) + n_tp - 1)

    buffers = {"mixed": mixed, "rest": rest}
    pieces = make_pieces(depth, mixed.shape[1], rest.shape[1])

    def copy(k, origin, link):
        p, r = pieces[k], at[origin]
        ref = buffers[p["buffer"]].at[
            pl.ds(pl.multiple_of(r * depth + p["row"], 16), p["rows"]),
            pl.ds(p["col"], p["cols"]),
        ]
        return pltpu.make_async_remote_copy(
            src_ref=ref,
            dst_ref=ref,
            send_sem=sent.at[p["phase"]],
            recv_sem=got.at[k, r],
            device_id={"rows": to[link]},
            device_id_type=MESH,
        )

    def norm_copy(ref, n, axis, index):
        return pltpu.make_async_remote_copy(
            src_ref=ref,
            dst_ref=ref,
            send_sem=sent_norm.at[n],
            recv_sem=got_norm.at[n],
            device_id={axis: index},
            device_id_type=MESH,
        )

    def peer_copy(d):
        return norm_copy(peers.at[t], d - 1, "tp", ts[d])

    def y_copy(n):
        dy, link = ((0, ("y", 1)), (0, ("y", -1)), (NY - 1, ("y", 1)))[n]
        return norm_copy(norms.at[pl.ds(at[dy, 0], 1)], 3 + n, "rows", to[link])

    def z_copy(n):
        dz, link = (-n % NZ, ("z", 1)) if n < 4 else (n - 4, ("z", -1))
        return norm_copy(norms.at[pl.ds(zs[dz] * NY, NY)], 6 + n, "rows", to[link])

    def norm_step_0():
        for d in range(1, n_tp):
            peer_copy(d).start()

    def norm_step_1():
        for d in range(1, n_tp):
            peer_copy(d).wait_recv()
        norms[rows] = sum(peers[d] for d in range(n_tp))

    def norm_step_2():
        y_copy(0).start()
        y_copy(1).start()

    def norm_step_3():
        y_copy(0).wait_recv()
        y_copy(2).start()
        y_copy(1).wait_recv()

    def norm_step_4():
        y_copy(2).wait_recv()
        z_copy(0).start()
        z_copy(4).start()

    def norm_hop(n):
        z_copy(n - 1).wait_recv()
        z_copy(n).start()
        if n < 3:
            z_copy(n + 3).wait_recv()
            z_copy(n + 4).start()

    def norm_last():
        z_copy(3).wait_recv()
        z_copy(6).wait_recv()
        n_norm = norms.shape[0] * share * n_tp
        lane = lax.broadcasted_iota(jnp.int32, (1, 128), 1)
        lines = [jnp.zeros((1, 128), jnp.float32) for _ in range(n_norm // 128)]
        width = share * n_tp
        for r in range(norms.shape[0]):
            line, off = divmod(r * width, 128)
            part = pltpu.roll(norms[r], off, 1) if off else norms[r]
            lines[line] += jnp.where(lane >= off, part, 0.0)
            if off + width > 128:
                lines[line + 1] += jnp.where(lane < off + width - 128, part, 0.0)
        norm_out[...] = jnp.concatenate(lines, axis=0).astype(norm_out.dtype)

    def turn(j):
        part = mixed[128 * j : 128 * (j + 1), :]
        mixed_out[:, 128 * j : 128 * (j + 1)] = part.T

    steps = plan(pieces)
    turned = [s[0] for s in steps if s[1] == "wait" and pieces[s[2]]["phase"] == 0][-1]
    end = steps[-1][0]
    n_turn = mixed.shape[0] // 128
    side_jobs = [(0.5, norm_step_0), (6.0, norm_step_1), (8.0, norm_step_2), (14.0, norm_step_3)]
    side_jobs += [(20.0, norm_step_4)]
    side_jobs += [(20.0 + 6.0 * n, functools.partial(norm_hop, n)) for n in range(1, 4)]
    side_jobs += [(46.0, norm_last)]
    gap = (end - 8.0 - turned) / n_turn
    side_jobs += [
        (turned + 0.01 + gap * j, functools.partial(turn, j)) for j in range(n_turn)
    ]
    side_jobs += [(min(s[0] for s in steps if pieces[s[2]]["phase"]) - 0.01, merge_rest)]
    side_jobs.sort(key=lambda job: job[0])

    for when, what, piece, origin, link in steps:
        while side_jobs and side_jobs[0][0] < when:
            side_jobs.pop(0)[1]()
        if what == "wait":
            copy(piece, origin, link).wait_recv()
        else:
            copy(piece, origin, link).start()
    for _, job in side_jobs:
        job()

    n_rows = mixed.shape[0]
    for phase, buffer in ((0, mixed), (1, rest)):
        others = buffer.at[pl.ds(0, n_rows - depth)]
        pltpu.make_async_remote_copy(
            src_ref=others,
            dst_ref=others,
            send_sem=sent.at[phase],
            recv_sem=got.at[0, 0],
            device_id={"rows": to["y", 1]},
            device_id_type=MESH,
        ).wait_send()
    for d in range(1, n_tp):
        peer_copy(d).wait_send()
    for n in range(3):
        y_copy(n).wait_send()
    for n in range(7):
        z_copy(n).wait_send()


def put_kernel(rest, mixed, norm, final_query, final_key, final_value, final_mixed, serve_norm, sems):
    q, k = final_query.shape[1], final_key.shape[1]
    moves = [(norm, serve_norm)]
    for source, final, cuts in (
        (mixed, final_mixed, 4),
        (rest.at[:, pl.ds(0, q)], final_query, 4),
        (rest.at[:, pl.ds(q, k)], final_key, 2),
        (rest.at[:, pl.ds(q + k, k)], final_value, 2),
    ):
        count = final.shape[0] // cuts
        for c in range(cuts):
            part = pl.ds(c * count, count)
            moves.append((source.at[part], final.at[part]))
    copies = [pltpu.make_async_copy(a, b, sems.at[n]) for n, (a, b) in enumerate(moves)]
    for c in copies:
        c.start()
    for c in copies:
        c.wait()


def shards(n_rows, n_tp, *args):
    (
        w_query,
        low_query,
        high_query,
        w_key,
        low_key,
        high_key,
        w_value,
        low_value,
        high_value,
        w_mixed,
        low_mixed,
        high_mixed,
        norm_train,
        norm_step,
    ) = args
    depth, q, k = w_query.shape[0], w_query.shape[1], w_key.shape[1]
    m = w_mixed.shape[0]
    total = n_rows * depth
    n_norm = n_rows * n_tp * norm_train.shape[0]
    bf16, f32 = jnp.bfloat16, jnp.float32
    vmem = pl.BlockSpec(memory_space=pltpu.VMEM)
    n_pieces = len(make_pieces(depth, m, q + 2 * k))
    hbm = pl.BlockSpec(memory_space=pltpu.HBM)
    given = (
        w_query,
        low_query.T,
        high_query,
        w_key,
        low_key.T,
        high_key,
        w_value,
        low_value.T,
        high_value,
        w_mixed.T,
        low_mixed.T,
        high_mixed,
        norm_train.reshape(1, -1),
        norm_step.reshape(1, -1),
    )
    made = pl.pallas_call(
        functools.partial(gather_kernel, n_tp, depth),
        out_shape=(
            pltpu.VMEM((total, q + 2 * k), bf16),
            pltpu.VMEM((m, total), bf16),
            pltpu.VMEM((n_norm // 128, 128), bf16),
        ),
        in_specs=[hbm] * N_ARGS,
        out_specs=(vmem, vmem, vmem),
        scratch_shapes=[
            *(pltpu.VMEM(a.shape, a.dtype) for a in given),
            pltpu.VMEM((total, m), bf16),
            pltpu.VMEM((n_tp, 1, 128), f32),
            pltpu.VMEM((n_rows, 1, 128), f32),
            pltpu.SemaphoreType.DMA((N_ARGS,)),
            pltpu.SemaphoreType.DMA((2,)),
            pltpu.SemaphoreType.DMA((n_pieces, n_rows)),
            pltpu.SemaphoreType.DMA((13,)),
            pltpu.SemaphoreType.DMA((13,)),
        ],
        compiler_params=pltpu.CompilerParams(
            collective_id=0, has_side_effects=True, vmem_limit_bytes=16 << 20
        ),
        name="gather",
    )(*(pltpu.with_memory_space_constraint(a, pltpu.HBM) for a in given))
    final_query, final_key, final_value, final_mixed, serve_norm = pl.pallas_call(
        put_kernel,
        out_shape=(
            jax.ShapeDtypeStruct((total, q), bf16),
            jax.ShapeDtypeStruct((total, k), bf16),
            jax.ShapeDtypeStruct((total, k), bf16),
            jax.ShapeDtypeStruct((m, total), bf16),
            jax.ShapeDtypeStruct((n_norm // 128, 128), bf16),
        ),
        in_specs=[vmem] * 3,
        out_specs=(hbm,) * 5,
        scratch_shapes=[pltpu.SemaphoreType.DMA((13,))],
        compiler_params=pltpu.CompilerParams(vmem_limit_bytes=2 << 20),
        name="put",
    )(*(pltpu.with_memory_space_constraint(a, pltpu.VMEM) for a in made))
    return final_query, final_key, final_value, final_mixed, serve_norm.reshape(-1)


def solution(mesh):
    return jax.shard_map(
        functools.partial(shards, mesh.shape["rows"], mesh.shape["tp"]),
        mesh=mesh,
        in_specs=(
            P(UNIT_ROWS, "tp"),
            P(UNIT_ROWS, None),
            P("unit", "tp"),
            P(UNIT_ROWS, "tp"),
            P(UNIT_ROWS, None),
            P("unit", "tp"),
            P(UNIT_ROWS, "tp"),
            P(UNIT_ROWS, None),
            P("unit", "tp"),
            P(("unit", "tp"), "rows"),
            P(("unit", "tp"), None),
            P("unit", "rows"),
            P(UNIT_ROWS_TP),
            P(UNIT_ROWS_TP),
        ),
        out_specs=(
            P("unit", "tp"),
            P("unit", "tp"),
            P("unit", "tp"),
            P(("unit", "tp"), None),
            P("unit"),
        ),
        check_vma=False,
    )
```

```python
import functools
import heapq

import jax
import jax.numpy as jnp
from jax import lax
from jax.experimental import pallas as pl
from jax.experimental.pallas import tpu as pltpu
from jax.sharding import PartitionSpec as P

MESH = pl.DeviceIdType.MESH
UNIT_ROWS = ("unit", "rows")
UNIT_ROWS_TP = ("unit", "rows", "tp")

mix_rate = 0.5
N_ARGS = 14

NY, NZ = 4, 8
SIZE = {"y": NY, "z": NZ}
LINKS = (("y", 1), ("y", -1), ("z", 1), ("z", -1))
RATE, LATENCY, LEAD = 46.6e3, 5.0, 6.0


def reach(n, step, side):
    return n // 2 if (side == 0) == (step > 0) else n - 1 - n // 2


def onward(piece, via, hops):
    first, second = ("y", "z") if piece["y_first"] else ("z", "y")
    if via is None:
        out = [((axis, step), 1) for axis in (first, second) for step in (1, -1)]
    else:
        out = [(via, hops + 1)]
        if via[0] == first:
            out += [((second, step), 1) for step in (1, -1)]
    return [(l, h) for l, h in out if h <= reach(SIZE[l[0]], l[1], piece["side"])]


def plan(pieces):
    def urgency(piece, link, hops):
        left = reach(SIZE[link[0]], link[1], piece["side"]) - hops
        first, second = ("y", "z") if piece["y_first"] else ("z", "y")
        return piece["phase"], -(left + (SIZE[second] // 2 if link[0] == first else 0))

    queue, free, seq = {l: [] for l in LINKS}, dict.fromkeys(LINKS, 0.0), 0
    events, steps, got, last = [], [], {}, dict.fromkeys(LINKS, 0.0)

    def hold(k, origin, via, hops):
        nonlocal seq
        for link, h in onward(pieces[k], via, hops):
            seq += 1
            heapq.heappush(queue[link], (urgency(pieces[k], link, h), seq, k, origin, h))

    for k in range(len(pieces)):
        got[k, (0, 0)] = 0.0
        hold(k, (0, 0), None, 0)
    now = 0.0
    while True:
        for link in LINKS:
            if free[link] <= now + 1e-9 and queue[link]:
                _, _, k, origin, h = heapq.heappop(queue[link])
                issue = max(got[k, origin], now - LEAD, last[link])
                last[link] = issue
                seq += 1
                steps.append((issue, seq, "send", k, origin, link))
                free[link] = now + pieces[k]["bytes"] / RATE
                dy, dz = origin
                there = ((dy - link[1]) % NY, dz) if link[0] == "y" else (dy, (dz - link[1]) % NZ)
                heapq.heappush(events, (free[link], seq, None))
                heapq.heappush(events, (free[link] + LATENCY, seq, (k, there, link, h)))
        if not events:
            break
        now = events[0][0]
        while events and events[0][0] <= now + 1e-9:
            _, _, landed = heapq.heappop(events)
            if landed is not None:
                k, origin, link, h = landed
                got[k, origin] = now
                seq += 1
                steps.append((now, seq, "wait", k, origin, link))
                hold(k, origin, link, h)
    steps.sort(key=lambda s: (s[0], s[2] == "send", s[1]))
    return [(t, *rest) for t, _, *rest in steps]


def make_pieces(depth, mixed, rest):
    pieces = []
    for phase, buffer, columns in ((0, "mixed", mixed), (1, "rest", rest)):
        cut = depth * 2 // 5 // 16 * 16
        for y_first, low, count in ((True, 0, cut), (False, cut, depth - cut)):
            for side in (0, 1):
                pieces.append(
                    dict(
                        phase=phase,
                        buffer=buffer,
                        y_first=y_first,
                        side=side,
                        row=low,
                        rows=count,
                        col=side * columns // 2,
                        cols=columns // 2,
                        bytes=count * columns,
                    )
                )
    return pieces


def merged(w, low_t, high):
    product = lax.dot_general(
        low_t, high, (((0,), (0,)), ((), ())), preferred_element_type=jnp.float32
    )
    return (w.astype(jnp.float32) + mix_rate * product).astype(jnp.bfloat16)


def gather_kernel(n_tp, depth, *refs):
    given, (rest, mixed_out, norm_out), held = refs[:N_ARGS], refs[N_ARGS : N_ARGS + 3], refs[N_ARGS + 3 :]
    fetched, (mixed, peers, norms, fetch_sem, sent, got, sent_norm, got_norm) = (
        held[:N_ARGS],
        held[N_ARGS:],
    )
    w_query, low_query, high_query, w_key, low_key, high_key, w_value, low_value, high_value = fetched[:9]
    w_mixed, low_mixed, high_mixed, norm_train, norm_step = fetched[9:]
    fetches = [
        pltpu.make_async_copy(a, b, fetch_sem.at[n])
        for n, (a, b) in enumerate(zip(given, fetched))
    ]
    for n in (*range(9, N_ARGS), *range(9)):
        fetches[n].start()

    rows, t = lax.axis_index("rows"), lax.axis_index("tp")
    z, y = rows // NY, lax.rem(rows, NY)
    ys = [lax.rem(y + d, NY) for d in range(NY)]
    zs = [lax.rem(z + d, NZ) for d in range(NZ)]
    ts = [lax.rem(t + d, n_tp) for d in range(n_tp)]
    at = {(dy, dz): zs[dz] * NY + ys[dy] for dy in range(NY) for dz in range(NZ)}
    to = {
        ("y", 1): at[1, 0],
        ("y", -1): at[NY - 1, 0],
        ("z", 1): at[0, 1],
        ("z", -1): at[0, NZ - 1],
    }

    barrier = pltpu.get_barrier_semaphore()
    for link in LINKS:
        pl.semaphore_signal(barrier, 1, device_id={"rows": to[link]}, device_id_type=MESH)
    for d in range(1, n_tp):
        pl.semaphore_signal(barrier, 1, device_id={"tp": ts[d]}, device_id_type=MESH)

    mine = pl.ds(pl.multiple_of(rows * depth, 16), depth)
    q, k = w_query.shape[1], w_key.shape[1]
    for n in range(9, N_ARGS):
        fetches[n].wait()
    mixed[mine, :] = merged(w_mixed[...], high_mixed[...], low_mixed[...])
    share = norm_train.shape[1]
    gain = norm_train[...] + norm_step[...]
    wide = jnp.concatenate([gain, jnp.zeros((1, 128 - share), jnp.float32)], axis=1)
    peers[t] = pltpu.roll(wide, t * share, 1)

    def merge_rest():
        for n in range(9):
            fetches[n].wait()
        rest[mine, :q] = merged(w_query[...], low_query[...], high_query[...])
        rest[mine, q : q + k] = merged(w_key[...], low_key[...], high_key[...])
        rest[mine, q + k :] = merged(w_value[...], low_value[...], high_value[...])

    pl.semaphore_wait(barrier, len(LINKS) + n_tp - 1)

    buffers = {"mixed": mixed, "rest": rest}
    pieces = make_pieces(depth, mixed.shape[1], rest.shape[1])

    def copy(k, origin, link):
        p, r = pieces[k], at[origin]
        ref = buffers[p["buffer"]].at[
            pl.ds(pl.multiple_of(r * depth + p["row"], 16), p["rows"]),
            pl.ds(p["col"], p["cols"]),
        ]
        return pltpu.make_async_remote_copy(
            src_ref=ref,
            dst_ref=ref,
            send_sem=sent.at[p["phase"]],
            recv_sem=got.at[k, r],
            device_id={"rows": to[link]},
            device_id_type=MESH,
        )

    def norm_copy(ref, n, axis, index):
        return pltpu.make_async_remote_copy(
            src_ref=ref,
            dst_ref=ref,
            send_sem=sent_norm.at[n],
            recv_sem=got_norm.at[n],
            device_id={axis: index},
            device_id_type=MESH,
        )

    def peer_copy(d):
        return norm_copy(peers.at[t], d - 1, "tp", ts[d])

    def y_copy(n):
        dy, link = ((0, ("y", 1)), (0, ("y", -1)), (NY - 1, ("y", 1)))[n]
        return norm_copy(norms.at[pl.ds(at[dy, 0], 1)], 3 + n, "rows", to[link])

    def z_copy(n):
        dz, link = (-n % NZ, ("z", 1)) if n < 4 else (n - 4, ("z", -1))
        return norm_copy(norms.at[pl.ds(zs[dz] * NY, NY)], 6 + n, "rows", to[link])

    def norm_step_0():
        for d in range(1, n_tp):
            peer_copy(d).start()

    def norm_step_1():
        for d in range(1, n_tp):
            peer_copy(d).wait_recv()
        norms[rows] = sum(peers[d] for d in range(n_tp))

    def norm_step_2():
        y_copy(0).start()
        y_copy(1).start()

    def norm_step_3():
        y_copy(0).wait_recv()
        y_copy(2).start()
        y_copy(1).wait_recv()

    def norm_step_4():
        y_copy(2).wait_recv()
        z_copy(0).start()
        z_copy(4).start()

    def norm_hop(n):
        z_copy(n - 1).wait_recv()
        z_copy(n).start()
        if n < 3:
            z_copy(n + 3).wait_recv()
            z_copy(n + 4).start()

    def norm_last():
        z_copy(3).wait_recv()
        z_copy(6).wait_recv()
        n_norm = norms.shape[0] * share * n_tp
        lane = lax.broadcasted_iota(jnp.int32, (1, 128), 1)
        lines = [jnp.zeros((1, 128), jnp.float32) for _ in range(n_norm // 128)]
        width = share * n_tp
        for r in range(norms.shape[0]):
            line, off = divmod(r * width, 128)
            part = pltpu.roll(norms[r], off, 1) if off else norms[r]
            lines[line] += jnp.where(lane >= off, part, 0.0)
            if off + width > 128:
                lines[line + 1] += jnp.where(lane < off + width - 128, part, 0.0)
        norm_out[...] = jnp.concatenate(lines, axis=0).astype(norm_out.dtype)

    def turn(j):
        part = mixed[128 * j : 128 * (j + 1), :]
        mixed_out[:, 128 * j : 128 * (j + 1)] = part.T

    steps = plan(pieces)
    turned = [s[0] for s in steps if s[1] == "wait" and pieces[s[2]]["phase"] == 0][-1]
    end = steps[-1][0]
    n_turn = mixed.shape[0] // 128
    side_jobs = [(0.5, norm_step_0), (6.0, norm_step_1), (8.0, norm_step_2), (14.0, norm_step_3)]
    side_jobs += [(20.0, norm_step_4)]
    side_jobs += [(20.0 + 6.0 * n, functools.partial(norm_hop, n)) for n in range(1, 4)]
    side_jobs += [(46.0, norm_last)]
    gap = (end - 8.0 - turned) / n_turn
    side_jobs += [
        (turned + 0.01 + gap * j, functools.partial(turn, j)) for j in range(n_turn)
    ]
    side_jobs += [(min(s[0] for s in steps if pieces[s[2]]["phase"]) - 0.01, merge_rest)]
    side_jobs.sort(key=lambda job: job[0])

    for when, what, piece, origin, link in steps:
        while side_jobs and side_jobs[0][0] < when:
            side_jobs.pop(0)[1]()
        if what == "wait":
            copy(piece, origin, link).wait_recv()
        else:
            copy(piece, origin, link).start()
    for _, job in side_jobs:
        job()

    n_rows = mixed.shape[0]
    for phase, buffer in ((0, mixed), (1, rest)):
        others = buffer.at[pl.ds(0, n_rows - depth)]
        pltpu.make_async_remote_copy(
            src_ref=others,
            dst_ref=others,
            send_sem=sent.at[phase],
            recv_sem=got.at[0, 0],
            device_id={"rows": to["y", 1]},
            device_id_type=MESH,
        ).wait_send()
    for d in range(1, n_tp):
        peer_copy(d).wait_send()
    for n in range(3):
        y_copy(n).wait_send()
    for n in range(7):
        z_copy(n).wait_send()


def put_kernel(rest, mixed, norm, final_query, final_key, final_value, final_mixed, serve_norm, sems):
    q, k = final_query.shape[1], final_key.shape[1]
    moves = [(norm, serve_norm)]
    for source, final, cuts in (
        (mixed, final_mixed, 4),
        (rest.at[:, pl.ds(0, q)], final_query, 4),
        (rest.at[:, pl.ds(q, k)], final_key, 2),
        (rest.at[:, pl.ds(q + k, k)], final_value, 2),
    ):
        count = final.shape[0] // cuts
        for c in range(cuts):
            part = pl.ds(c * count, count)
            moves.append((source.at[part], final.at[part]))
    copies = [pltpu.make_async_copy(a, b, sems.at[n]) for n, (a, b) in enumerate(moves)]
    for c in copies:
        c.start()
    for c in copies:
        c.wait()


def shards(n_rows, n_tp, *args):
    (
        w_query,
        low_query,
        high_query,
        w_key,
        low_key,
        high_key,
        w_value,
        low_value,
        high_value,
        w_mixed,
        low_mixed,
        high_mixed,
        norm_train,
        norm_step,
    ) = args
    depth, q, k = w_query.shape[0], w_query.shape[1], w_key.shape[1]
    m = w_mixed.shape[0]
    total = n_rows * depth
    n_norm = n_rows * n_tp * norm_train.shape[0]
    bf16, f32 = jnp.bfloat16, jnp.float32
    vmem = pl.BlockSpec(memory_space=pltpu.VMEM)
    n_pieces = len(make_pieces(depth, m, q + 2 * k))
    hbm = pl.BlockSpec(memory_space=pltpu.HBM)
    given = (
        w_query,
        low_query.T,
        high_query,
        w_key,
        low_key.T,
        high_key,
        w_value,
        low_value.T,
        high_value,
        w_mixed.T,
        low_mixed.T,
        high_mixed,
        norm_train.reshape(1, -1),
        norm_step.reshape(1, -1),
    )
    made = pl.pallas_call(
        functools.partial(gather_kernel, n_tp, depth),
        out_shape=(
            pltpu.VMEM((total, q + 2 * k), bf16),
            pltpu.VMEM((m, total), bf16),
            pltpu.VMEM((n_norm // 128, 128), bf16),
        ),
        in_specs=[hbm] * N_ARGS,
        out_specs=(vmem, vmem, vmem),
        scratch_shapes=[
            *(pltpu.VMEM(a.shape, a.dtype) for a in given),
            pltpu.VMEM((total, m), bf16),
            pltpu.VMEM((n_tp, 1, 128), f32),
            pltpu.VMEM((n_rows, 1, 128), f32),
            pltpu.SemaphoreType.DMA((N_ARGS,)),
            pltpu.SemaphoreType.DMA((2,)),
            pltpu.SemaphoreType.DMA((n_pieces, n_rows)),
            pltpu.SemaphoreType.DMA((13,)),
            pltpu.SemaphoreType.DMA((13,)),
        ],
        compiler_params=pltpu.CompilerParams(
            collective_id=0, has_side_effects=True, vmem_limit_bytes=16 << 20
        ),
        name="gather",
    )(*(pltpu.with_memory_space_constraint(a, pltpu.HBM) for a in given))
    final_query, final_key, final_value, final_mixed, serve_norm = pl.pallas_call(
        put_kernel,
        out_shape=(
            jax.ShapeDtypeStruct((total, q), bf16),
            jax.ShapeDtypeStruct((total, k), bf16),
            jax.ShapeDtypeStruct((total, k), bf16),
            jax.ShapeDtypeStruct((m, total), bf16),
            jax.ShapeDtypeStruct((n_norm // 128, 128), bf16),
        ),
        in_specs=[vmem] * 3,
        out_specs=(hbm,) * 5,
        scratch_shapes=[pltpu.SemaphoreType.DMA((13,))],
        compiler_params=pltpu.CompilerParams(vmem_limit_bytes=2 << 20),
        name="put",
    )(*(pltpu.with_memory_space_constraint(a, pltpu.VMEM) for a in made))
    return final_query, final_key, final_value, final_mixed, serve_norm.reshape(-1)


def solution(mesh):
    return jax.shard_map(
        functools.partial(shards, mesh.shape["rows"], mesh.shape["tp"]),
        mesh=mesh,
        in_specs=(
            P(UNIT_ROWS, "tp"),
            P(UNIT_ROWS, None),
            P("unit", "tp"),
            P(UNIT_ROWS, "tp"),
            P(UNIT_ROWS, None),
            P("unit", "tp"),
            P(UNIT_ROWS, "tp"),
            P(UNIT_ROWS, None),
            P("unit", "tp"),
            P(("unit", "tp"), "rows"),
            P(("unit", "tp"), None),
            P("unit", "rows"),
            P(UNIT_ROWS_TP),
            P(UNIT_ROWS_TP),
        ),
        out_specs=(
            P("unit", "tp"),
            P("unit", "tp"),
            P("unit", "tp"),
            P(("unit", "tp"), None),
            P("unit"),
        ),
        check_vma=False,
    )
```

```python
import functools
import heapq

import jax
import jax.numpy as jnp
from jax import lax
from jax.experimental import pallas as pl
from jax.experimental.pallas import tpu as pltpu
from jax.sharding import PartitionSpec as P

MESH = pl.DeviceIdType.MESH
UNIT_ROWS = ("unit", "rows")
UNIT_ROWS_TP = ("unit", "rows", "tp")

mix_rate = 0.5
N_ARGS = 14

NY, NZ = 4, 8
SIZE = {"y": NY, "z": NZ}
LINKS = (("y", 1), ("y", -1), ("z", 1), ("z", -1))
RATE, LATENCY, LEAD = 46.6e3, 6.5, 7.5


DETOUR = {("rest", True, 0): (0, 1)}
DETOURED = NZ // 2
HOLD = 5.0


def reach(n, step, side):
    return n // 2 if (side == 0) == (step > 0) else n - 1 - n // 2


def onward(piece, via, hops):
    first, second = ("y", "z") if piece["y_first"] else ("z", "y")
    if via is None:
        out = [((axis, step), 1) for axis in (first, second) for step in (1, -1)]
    else:
        out = [(via, hops + 1)]
        if via[0] == first:
            out += [((second, step), 1) for step in (1, -1)]
    return [(l, h) for l, h in out if h <= reach(SIZE[l[0]], l[1], piece["side"])]


def plan(pieces):
    def urgency(piece, link, hops):
        left = reach(SIZE[link[0]], link[1], piece["side"]) - hops
        first, second = ("y", "z") if piece["y_first"] else ("z", "y")
        return piece["phase"], -(left + (SIZE[second] // 2 if link[0] == first else 0))

    queue, free, seq = {l: [] for l in LINKS}, dict.fromkeys(LINKS, 0.0), 0
    events, steps, got, last = [], [], {}, dict.fromkeys(LINKS, 0.0)

    def hold(k, origin, via, hops):
        nonlocal seq
        for link, h in onward(pieces[k], via, hops):
            seq += 1
            heapq.heappush(queue[link], (urgency(pieces[k], link, h), seq, k, origin, h))

    for k in range(len(pieces)):
        got[k, (0, 0)] = 0.0
        hold(k, (0, 0), None, 0)
    now = 0.0
    while True:
        for link in LINKS:
            if free[link] <= now + 1e-9 and queue[link]:
                _, _, k, origin, h = heapq.heappop(queue[link])
                issue = max(got[k, origin], now - LEAD, last[link])
                last[link] = issue
                seq += 1
                steps.append((issue, seq, "send", k, origin, link))
                free[link] = now + pieces[k]["bytes"] / RATE
                dy, dz = origin
                there = ((dy - link[1]) % NY, dz) if link[0] == "y" else (dy, (dz - link[1]) % NZ)
                heapq.heappush(events, (free[link], seq, None))
                heapq.heappush(events, (free[link] + LATENCY, seq, (k, there, link, h)))
        if not events:
            break
        now = events[0][0]
        while events and events[0][0] <= now + 1e-9:
            _, _, landed = heapq.heappop(events)
            if landed is not None:
                k, origin, link, h = landed
                got[k, origin] = now
                seq += 1
                steps.append((now, seq, "wait", k, origin, link))
                hold(k, origin, link, h)
    steps.sort(key=lambda s: (s[0], s[2] == "send", s[1]))
    return [(t, *rest) for t, _, *rest in steps]


def with_detours(steps, pieces):
    steps, tail = [(*s, None) for s in steps], []
    for k, piece in enumerate(pieces):
        step = 1 if piece["side"] == 0 else -1
        near, far = step * (NZ // 2 - 1) % NZ, -step * (NZ // 2 - 1) % NZ
        for dy in piece["detour"]:
            what = [s[1:5] for s in steps]
            usual = what.index(("send", k, (dy, far), ("z", step)))
            ready = [w[:3] for w in what].index(("wait", k, (dy, near)))
            steps[usual] = (*steps[usual][:5], False)
            at = max(usual, ready)
            steps.insert(at + 1, (steps[at][0], "send", k, (dy, near), ("z", -step), True))
            last = [s[1:4] for s in steps].index(("wait", k, (dy, NZ // 2)))
            tail.append(steps.pop(last))
    return steps + tail


def make_pieces(depth, mixed, rest):
    pieces = []
    for phase, buffer, columns in ((0, "mixed", mixed), (1, "rest", rest)):
        cut = depth * 2 // 5 // 16 * 16
        for y_first, low, count in ((True, 0, cut), (False, cut, depth - cut)):
            for side in (0, 1):
                pieces.append(
                    dict(
                        phase=phase,
                        buffer=buffer,
                        y_first=y_first,
                        side=side,
                        row=low,
                        rows=count,
                        col=side * columns // 2,
                        cols=columns // 2,
                        bytes=count * columns,
                        detour=DETOUR.get((buffer, y_first, side), ()),
                    )
                )
    return pieces


def merged(w, low_t, high):
    product = lax.dot_general(
        low_t, high, (((0,), (0,)), ((), ())), preferred_element_type=jnp.float32
    )
    return (w.astype(jnp.float32) + mix_rate * product).astype(jnp.bfloat16)


def gather_kernel(n_tp, depth, *refs):
    given, (rest, mixed_out, norm_out), held = refs[:N_ARGS], refs[N_ARGS : N_ARGS + 3], refs[N_ARGS + 3 :]
    fetched, (mixed, peers, norms, fetch_sem, late, sent, sent_some, got, sent_norm, got_norm) = (
        held[:N_ARGS],
        held[N_ARGS:],
    )
    w_query, low_query, high_query, w_key, low_key, high_key, w_value, low_value, high_value = fetched[:9]
    w_mixed, low_mixed, high_mixed, norm_train, norm_step = fetched[9:]
    fetches = [
        pltpu.make_async_copy(a, b, fetch_sem.at[n])
        for n, (a, b) in enumerate(zip(given, fetched))
    ]
    for n in (*range(9, N_ARGS), *range(9)):
        fetches[n].start()

    rows, t = lax.axis_index("rows"), lax.axis_index("tp")
    z, y = rows // NY, lax.rem(rows, NY)
    ys = [lax.rem(y + d, NY) for d in range(NY)]
    zs = [lax.rem(z + d, NZ) for d in range(NZ)]
    ts = [lax.rem(t + d, n_tp) for d in range(n_tp)]
    at = {(dy, dz): zs[dz] * NY + ys[dy] for dy in range(NY) for dz in range(NZ)}
    to = {
        ("y", 1): at[1, 0],
        ("y", -1): at[NY - 1, 0],
        ("z", 1): at[0, 1],
        ("z", -1): at[0, NZ - 1],
    }

    barrier = pltpu.get_barrier_semaphore()
    first_z, last_z = z == 0, z == NZ - 1

    def greet(link, semaphore=barrier):
        pl.semaphore_signal(semaphore, 1, device_id={"rows": to[link]}, device_id_type=MESH)

    for link in LINKS:
        if link == ("z", 1):
            pl.when(jnp.logical_not(last_z))(functools.partial(greet, link))
        else:
            greet(link)
    for d in range(1, n_tp):
        pl.semaphore_signal(barrier, 1, device_id={"tp": ts[d]}, device_id_type=MESH)

    mine = pl.ds(pl.multiple_of(rows * depth, 16), depth)
    q, k = w_query.shape[1], w_key.shape[1]
    for n in range(9, N_ARGS):
        fetches[n].wait()
    mixed[mine, :] = merged(w_mixed[...], high_mixed[...], low_mixed[...])
    share = norm_train.shape[1]
    gain = norm_train[...] + norm_step[...]
    wide = jnp.concatenate([gain, jnp.zeros((1, 128 - share), jnp.float32)], axis=1)
    peers[t] = pltpu.roll(wide, t * share, 1)

    def merge_rest():
        for n in range(9):
            fetches[n].wait()
        rest[mine, :q] = merged(w_query[...], low_query[...], high_query[...])
        rest[mine, q : q + k] = merged(w_key[...], low_key[...], high_key[...])
        rest[mine, q + k :] = merged(w_value[...], low_value[...], high_value[...])

    pl.semaphore_wait(barrier, len(LINKS) + n_tp - 1 - first_z.astype(jnp.int32))
    pl.when(last_z)(functools.partial(greet, ("z", 1), late))

    buffers = {"mixed": mixed, "rest": rest}
    pieces = make_pieces(depth, mixed.shape[1], rest.shape[1])

    def copy(k, origin, link, sent_by=None):
        p, r = pieces[k], at[origin]
        ref = buffers[p["buffer"]].at[
            pl.ds(pl.multiple_of(r * depth + p["row"], 16), p["rows"]),
            pl.ds(p["col"], p["cols"]),
        ]
        return pltpu.make_async_remote_copy(
            src_ref=ref,
            dst_ref=ref,
            send_sem=sent.at[p["phase"]] if sent_by is None else sent_some.at[sent_by],
            recv_sem=got.at[k, r],
            device_id={"rows": to[link]},
            device_id_type=MESH,
        )

    def norm_copy(ref, n, axis, index):
        return pltpu.make_async_remote_copy(
            src_ref=ref,
            dst_ref=ref,
            send_sem=sent_norm.at[n],
            recv_sem=got_norm.at[n],
            device_id={axis: index},
            device_id_type=MESH,
        )

    def peer_copy(d):
        return norm_copy(peers.at[t], d - 1, "tp", ts[d])

    def y_copy(n):
        dy, link = ((0, ("y", 1)), (0, ("y", -1)), (NY - 1, ("y", 1)))[n]
        return norm_copy(norms.at[pl.ds(at[dy, 0], 1)], 3 + n, "rows", to[link])

    def z_copy(n):
        dz, link = (-n % NZ, ("z", 1)) if n < 4 else (n - 4, ("z", -1))
        return norm_copy(norms.at[pl.ds(zs[dz] * NY, NY)], 6 + n, "rows", to[link])

    def norm_step_0():
        for d in range(1, n_tp):
            peer_copy(d).start()

    def norm_step_1():
        for d in range(1, n_tp):
            peer_copy(d).wait_recv()
        norms[rows] = sum(peers[d] for d in range(n_tp))

    def norm_step_2():
        y_copy(0).start()
        y_copy(1).start()

    def norm_step_3():
        y_copy(0).wait_recv()
        y_copy(2).start()
        y_copy(1).wait_recv()

    def norm_step_4():
        y_copy(2).wait_recv()
        z_copy(0).start()
        z_copy(4).start()

    def norm_hop(n):
        z_copy(n - 1).wait_recv()
        z_copy(n).start()
        if n < 3:
            z_copy(n + 3).wait_recv()
            z_copy(n + 4).start()

    def norm_last():
        z_copy(3).wait_recv()
        z_copy(6).wait_recv()
        n_norm = norms.shape[0] * share * n_tp
        lane = lax.broadcasted_iota(jnp.int32, (1, 128), 1)
        lines = [jnp.zeros((1, 128), jnp.float32) for _ in range(n_norm // 128)]
        width = share * n_tp
        for r in range(norms.shape[0]):
            line, off = divmod(r * width, 128)
            part = pltpu.roll(norms[r], off, 1) if off else norms[r]
            lines[line] += jnp.where(lane >= off, part, 0.0)
            if off + width > 128:
                lines[line + 1] += jnp.where(lane < off + width - 128, part, 0.0)
        norm_out[...] = jnp.concatenate(lines, axis=0).astype(norm_out.dtype)

    def turn(j):
        part = mixed[128 * j : 128 * (j + 1), :]
        mixed_out[:, 128 * j : 128 * (j + 1)] = part.T

    steps = with_detours(plan(pieces), pieces)
    turned = [s[0] for s in steps if s[1] == "wait" and pieces[s[2]]["phase"] == 0][-1]
    end = steps[-1][0]
    n_turn = mixed.shape[0] // 128
    side_jobs = [(0.5, norm_step_0), (6.0, norm_step_1), (8.0, norm_step_2), (14.0, norm_step_3)]
    side_jobs += [(20.0, norm_step_4)]
    side_jobs += [(20.0 + 6.0 * n, functools.partial(norm_hop, n)) for n in range(1, 4)]
    side_jobs += [(46.0, norm_last)]
    gap = (end - 8.0 - turned) / n_turn
    side_jobs += [
        (turned + 0.01 + gap * j, functools.partial(turn, j)) for j in range(n_turn)
    ]
    side_jobs += [(min(s[0] for s in steps if pieces[s[2]]["phase"]) - 0.01, merge_rest)]
    side_jobs.sort(key=lambda job: job[0])

    first = [s[0] >= HOLD or s[1] == "wait" for s in steps].index(True)
    down = ("z", -1)
    held = [copy(*s[2:5]) for s in steps[:first] if s[4] == down]

    def begin_down():
        pl.semaphore_wait(late, 1)
        for c in held:
            c.start()

    conditional = []
    for n, (when, what, piece, origin, link, detour) in enumerate(steps):
        while side_jobs and side_jobs[0][0] < when:
            side_jobs.pop(0)[1]()
        if n == first:
            pl.when(first_z)(begin_down)
        if what == "wait":
            copy(piece, origin, link).wait_recv()
        elif n < first and link == down:
            pl.when(jnp.logical_not(first_z))(copy(piece, origin, link).start)
        elif detour is None:
            copy(piece, origin, link).start()
        else:
            own = zs[origin[1]]
            hit = own == DETOURED if detour else own != DETOURED
            some = copy(piece, origin, link, len(conditional))
            pl.when(hit)(some.start)
            conditional.append((hit, some))
    for _, job in side_jobs:
        job()

    for hit, some in conditional:
        pl.when(hit)(some.wait_send)
    for phase, buffer in ((0, mixed), (1, rest)):
        other = buffer.shape[0] - depth
        for p in pieces:
            if p["phase"] == phase and p["detour"]:
                other -= len(p["detour"]) * p["rows"] * p["cols"] // buffer.shape[1]
        area = buffer.at[pl.ds(0, other)]
        pltpu.make_async_remote_copy(
            src_ref=area,
            dst_ref=area,
            send_sem=sent.at[phase],
            recv_sem=got.at[0, 0],
            device_id={"rows": to["y", 1]},
            device_id_type=MESH,
        ).wait_send()
    for d in range(1, n_tp):
        peer_copy(d).wait_send()
    for n in range(3):
        y_copy(n).wait_send()
    for n in range(7):
        z_copy(n).wait_send()


def put_kernel(rest, mixed, norm, final_query, final_key, final_value, final_mixed, serve_norm, sems):
    q, k = final_query.shape[1], final_key.shape[1]
    moves = [(norm, serve_norm)]
    for source, final, cuts in (
        (mixed, final_mixed, 4),
        (rest.at[:, pl.ds(0, q)], final_query, 4),
        (rest.at[:, pl.ds(q, k)], final_key, 2),
        (rest.at[:, pl.ds(q + k, k)], final_value, 2),
    ):
        count = final.shape[0] // cuts
        for c in range(cuts):
            part = pl.ds(c * count, count)
            moves.append((source.at[part], final.at[part]))
    copies = [pltpu.make_async_copy(a, b, sems.at[n]) for n, (a, b) in enumerate(moves)]
    for c in copies:
        c.start()
    for c in copies:
        c.wait()


def shards(n_rows, n_tp, *args):
    (
        w_query,
        low_query,
        high_query,
        w_key,
        low_key,
        high_key,
        w_value,
        low_value,
        high_value,
        w_mixed,
        low_mixed,
        high_mixed,
        norm_train,
        norm_step,
    ) = args
    depth, q, k = w_query.shape[0], w_query.shape[1], w_key.shape[1]
    m = w_mixed.shape[0]
    total = n_rows * depth
    n_norm = n_rows * n_tp * norm_train.shape[0]
    bf16, f32 = jnp.bfloat16, jnp.float32
    vmem = pl.BlockSpec(memory_space=pltpu.VMEM)
    n_pieces = len(make_pieces(depth, m, q + 2 * k))
    hbm = pl.BlockSpec(memory_space=pltpu.HBM)
    given = (
        w_query,
        low_query.T,
        high_query,
        w_key,
        low_key.T,
        high_key,
        w_value,
        low_value.T,
        high_value,
        w_mixed.T,
        low_mixed.T,
        high_mixed,
        norm_train.reshape(1, -1),
        norm_step.reshape(1, -1),
    )
    made = pl.pallas_call(
        functools.partial(gather_kernel, n_tp, depth),
        out_shape=(
            pltpu.VMEM((total, q + 2 * k), bf16),
            pltpu.VMEM((m, total), bf16),
            pltpu.VMEM((n_norm // 128, 128), bf16),
        ),
        in_specs=[hbm] * N_ARGS,
        out_specs=(vmem, vmem, vmem),
        scratch_shapes=[
            *(pltpu.VMEM(a.shape, a.dtype) for a in given),
            pltpu.VMEM((total, m), bf16),
            pltpu.VMEM((n_tp, 1, 128), f32),
            pltpu.VMEM((n_rows, 1, 128), f32),
            pltpu.SemaphoreType.DMA((N_ARGS,)),
            pltpu.SemaphoreType.REGULAR,
            pltpu.SemaphoreType.DMA((2,)),
            pltpu.SemaphoreType.DMA((2 * sum(len(d) for d in DETOUR.values()),)),
            pltpu.SemaphoreType.DMA((n_pieces, n_rows)),
            pltpu.SemaphoreType.DMA((13,)),
            pltpu.SemaphoreType.DMA((13,)),
        ],
        compiler_params=pltpu.CompilerParams(
            collective_id=0, has_side_effects=True, vmem_limit_bytes=16 << 20
        ),
        name="gather",
    )(*(pltpu.with_memory_space_constraint(a, pltpu.HBM) for a in given))
    final_query, final_key, final_value, final_mixed, serve_norm = pl.pallas_call(
        put_kernel,
        out_shape=(
            jax.ShapeDtypeStruct((total, q), bf16),
            jax.ShapeDtypeStruct((total, k), bf16),
            jax.ShapeDtypeStruct((total, k), bf16),
            jax.ShapeDtypeStruct((m, total), bf16),
            jax.ShapeDtypeStruct((n_norm // 128, 128), bf16),
        ),
        in_specs=[vmem] * 3,
        out_specs=(hbm,) * 5,
        scratch_shapes=[pltpu.SemaphoreType.DMA((13,))],
        compiler_params=pltpu.CompilerParams(vmem_limit_bytes=2 << 20),
        name="put",
    )(*(pltpu.with_memory_space_constraint(a, pltpu.VMEM) for a in made))
    return final_query, final_key, final_value, final_mixed, serve_norm.reshape(-1)


def solution(mesh):
    return jax.shard_map(
        functools.partial(shards, mesh.shape["rows"], mesh.shape["tp"]),
        mesh=mesh,
        in_specs=(
            P(UNIT_ROWS, "tp"),
            P(UNIT_ROWS, None),
            P("unit", "tp"),
            P(UNIT_ROWS, "tp"),
            P(UNIT_ROWS, None),
            P("unit", "tp"),
            P(UNIT_ROWS, "tp"),
            P(UNIT_ROWS, None),
            P("unit", "tp"),
            P(("unit", "tp"), "rows"),
            P(("unit", "tp"), None),
            P("unit", "rows"),
            P(UNIT_ROWS_TP),
            P(UNIT_ROWS_TP),
        ),
        out_specs=(
            P("unit", "tp"),
            P("unit", "tp"),
            P("unit", "tp"),
            P(("unit", "tp"), None),
            P("unit"),
        ),
        check_vma=False,
    )
```

```python
import functools
import heapq

import jax
import jax.numpy as jnp
from jax import lax
from jax.experimental import pallas as pl
from jax.experimental.pallas import tpu as pltpu
from jax.sharding import PartitionSpec as P

MESH = pl.DeviceIdType.MESH
UNIT_ROWS = ("unit", "rows")
UNIT_ROWS_TP = ("unit", "rows", "tp")

mix_rate = 0.5
N_ARGS = 14

NY, NZ = 4, 8
SIZE = {"y": NY, "z": NZ}
LINKS = (("y", 1), ("y", -1), ("z", 1), ("z", -1))
RATE, LATENCY, LEAD = 46.6e3, 6.5, 7.5


DETOUR = {("rest", True, 0): (0, 1)}
DETOURED = NZ // 2
PAIRS = True
HOLD = 5.0


def reach(n, step, side):
    return n // 2 if (side == 0) == (step > 0) else n - 1 - n // 2


def onward(piece, via, hops):
    first, second = ("y", "z") if piece["y_first"] else ("z", "y")
    if via is None:
        out = [((axis, step), 1) for axis in (first, second) for step in (1, -1)]
    else:
        out = [(via, hops + 1)]
        if via[0] == first:
            out += [((second, step), 1) for step in (1, -1)]
    return [(l, h) for l, h in out if h <= reach(SIZE[l[0]], l[1], piece["side"])]


def slot_of(pieces, k, origin):
    piece, (dy, dz) = pieces[k], origin
    detoured = dy in piece["detour"] and dz == (NZ // 2 - 1 if piece["side"] == 0 else NZ // 2 + 1)
    if not onward(piece, *way_of(piece, origin)) and not detoured:
        return "last", piece["phase"]
    if PAIRS and piece["y_first"] and dz in (1, 2, NZ - 2, NZ - 1):
        return k - k % 2, origin
    return k, origin


def way_of(piece, origin):
    dy, dz = origin
    axis = "z" if dz and (piece["y_first"] or not dy) else "y"
    n, off = SIZE[axis], dz if axis == "z" else dy
    if n - off <= reach(n, 1, piece["side"]):
        return (axis, 1), n - off
    return (axis, -1), off


def plan(pieces):
    def urgency(piece, link, hops):
        left = reach(SIZE[link[0]], link[1], piece["side"]) - hops
        first, second = ("y", "z") if piece["y_first"] else ("z", "y")
        return piece["phase"], -(left + (SIZE[second] // 2 if link[0] == first else 0))

    queue, free, seq = {l: [] for l in LINKS}, dict.fromkeys(LINKS, 0.0), 0
    events, steps, got, ready, last = [], [], {}, {}, dict.fromkeys(LINKS, 0.0)
    everywhere = [(k, (dy, dz)) for k in range(len(pieces)) for dy in range(NY) for dz in range(NZ) if dy or dz]
    slots = {}
    for k, origin in everywhere:
        slots.setdefault(slot_of(pieces, k, origin), []).append((k, origin))

    def hold(k, origin, via, hops):
        nonlocal seq
        for link, h in onward(pieces[k], via, hops):
            seq += 1
            heapq.heappush(queue[link], (urgency(pieces[k], link, h), seq, k, origin, h))

    for k in range(len(pieces)):
        ready[k, (0, 0)] = 0.0
        hold(k, (0, 0), None, 0)
    now = 0.0
    while True:
        for link in LINKS:
            if free[link] <= now + 1e-9 and queue[link]:
                _, _, k, origin, h = heapq.heappop(queue[link])
                issue = max(ready[k, origin], now - LEAD, last[link])
                last[link] = issue
                seq += 1
                steps.append((issue, seq, "send", k, origin, link))
                free[link] = now + pieces[k]["bytes"] / RATE
                heapq.heappush(events, (free[link], seq, None))
                heapq.heappush(events, (free[link] + LATENCY, seq, (k, beyond(origin, link), link, h)))
        if not events:
            break
        now = events[0][0]
        while events and events[0][0] <= now + 1e-9:
            _, _, landed = heapq.heappop(events)
            if landed is not None:
                k, origin, link, h = landed
                got[k, origin] = link, h
                slot = slot_of(pieces, k, origin)
                if all(one in got for one in slots[slot]):
                    seq += 1
                    steps.append((now, seq, "wait", slot, None, None))
                    for one in slots[slot]:
                        hold(*one, *got[one])
                        ready[one] = now
    steps.sort(key=lambda s: (s[0], s[2] == "send", s[1]))
    return [(t, *rest) for t, _, *rest in steps], slots


def beyond(origin, link):
    (dy, dz), (axis, step) = origin, link
    return ((dy - step) % NY, dz) if axis == "y" else (dy, (dz - step) % NZ)


def with_detours(steps, pieces, slots):
    steps = [(*s, None) for s in steps]
    for k, piece in enumerate(pieces):
        step = 1 if piece["side"] == 0 else -1
        near, far = step * (NZ // 2 - 1) % NZ, -step * (NZ // 2 - 1) % NZ
        for dy in piece["detour"]:
            what = [s[1:5] for s in steps]
            usual = what.index(("send", k, (dy, far), ("z", step)))
            slot = slot_of(pieces, k, (dy, near))
            at = max(usual, [w[:2] for w in what].index(("wait", slot)))
            steps[usual] = (*steps[usual][:5], False)
            steps.insert(at + 1, (steps[at][0], "send", k, (dy, near), ("z", -step), True))
    return steps


def make_pieces(depth, mixed, rest):
    pieces = []
    for phase, buffer, columns in ((0, "mixed", mixed), (1, "rest", rest)):
        cut = depth * 2 // 5 // 16 * 16
        for y_first, low, count in ((True, 0, cut), (False, cut, depth - cut)):
            for side in (0, 1):
                pieces.append(
                    dict(
                        phase=phase,
                        buffer=buffer,
                        y_first=y_first,
                        side=side,
                        row=low,
                        rows=count,
                        col=side * columns // 2,
                        cols=columns // 2,
                        bytes=count * columns,
                        detour=DETOUR.get((buffer, y_first, side), ()),
                    )
                )
    return pieces


def merged(w, low_t, high):
    product = lax.dot_general(
        low_t, high, (((0,), (0,)), ((), ())), preferred_element_type=jnp.float32
    )
    return (w.astype(jnp.float32) + mix_rate * product).astype(jnp.bfloat16)


def gather_kernel(n_tp, depth, *refs):
    given, (rest, mixed_out, norm_out), held = refs[:N_ARGS], refs[N_ARGS : N_ARGS + 3], refs[N_ARGS + 3 :]
    fetched, (mixed, peers, norms, fetch_sem, late, sent, sent_some, got, sent_norm, got_norm) = (
        held[:N_ARGS],
        held[N_ARGS:],
    )
    w_query, low_query, high_query, w_key, low_key, high_key, w_value, low_value, high_value = fetched[:9]
    w_mixed, low_mixed, high_mixed, norm_train, norm_step = fetched[9:]
    fetches = [
        pltpu.make_async_copy(a, b, fetch_sem.at[n])
        for n, (a, b) in enumerate(zip(given, fetched))
    ]
    for n in (*range(9, N_ARGS), *range(9)):
        fetches[n].start()

    rows, t = lax.axis_index("rows"), lax.axis_index("tp")
    z, y = rows // NY, lax.rem(rows, NY)
    ys = [lax.rem(y + d, NY) for d in range(NY)]
    zs = [lax.rem(z + d, NZ) for d in range(NZ)]
    ts = [lax.rem(t + d, n_tp) for d in range(n_tp)]
    at = {(dy, dz): zs[dz] * NY + ys[dy] for dy in range(NY) for dz in range(NZ)}
    to = {
        ("y", 1): at[1, 0],
        ("y", -1): at[NY - 1, 0],
        ("z", 1): at[0, 1],
        ("z", -1): at[0, NZ - 1],
    }

    barrier = pltpu.get_barrier_semaphore()
    first_z, last_z = z == 0, z == NZ - 1

    def greet(link, semaphore=barrier):
        pl.semaphore_signal(semaphore, 1, device_id={"rows": to[link]}, device_id_type=MESH)

    for link in LINKS:
        if link == ("z", 1):
            pl.when(jnp.logical_not(last_z))(functools.partial(greet, link))
        else:
            greet(link)
    for d in range(1, n_tp):
        pl.semaphore_signal(barrier, 1, device_id={"tp": ts[d]}, device_id_type=MESH)

    mine = pl.ds(pl.multiple_of(rows * depth, 16), depth)
    q, k = w_query.shape[1], w_key.shape[1]
    for n in range(9, N_ARGS):
        fetches[n].wait()
    mixed[mine, :] = merged(w_mixed[...], high_mixed[...], low_mixed[...])
    share = norm_train.shape[1]
    gain = norm_train[...] + norm_step[...]
    wide = jnp.concatenate([gain, jnp.zeros((1, 128 - share), jnp.float32)], axis=1)
    peers[t] = pltpu.roll(wide, t * share, 1)

    def merge_rest():
        for n in range(9):
            fetches[n].wait()
        rest[mine, :q] = merged(w_query[...], low_query[...], high_query[...])
        rest[mine, q : q + k] = merged(w_key[...], low_key[...], high_key[...])
        rest[mine, q + k :] = merged(w_value[...], low_value[...], high_value[...])

    pl.semaphore_wait(barrier, len(LINKS) + n_tp - 1 - first_z.astype(jnp.int32))
    pl.when(last_z)(functools.partial(greet, ("z", 1), late))

    buffers = {"mixed": mixed, "rest": rest}
    pieces = make_pieces(depth, mixed.shape[1], rest.shape[1])

    steps, slots = plan(pieces)
    steps = with_detours(steps, pieces, slots)
    numbers = {slot: n for n, slot in enumerate(slots)}

    def copy(k, origin, link, sent_by=None):
        p, r = pieces[k], at[origin]
        ref = buffers[p["buffer"]].at[
            pl.ds(pl.multiple_of(r * depth + p["row"], 16), p["rows"]),
            pl.ds(p["col"], p["cols"]),
        ]
        return pltpu.make_async_remote_copy(
            src_ref=ref,
            dst_ref=ref,
            send_sem=sent.at[p["phase"]] if sent_by is None else sent_some.at[sent_by],
            recv_sem=got.at[numbers[slot_of(pieces, k, beyond(origin, link))]],
            device_id={"rows": to[link]},
            device_id_type=MESH,
        )

    def arrival(slot):
        p = pieces[slots[slot][0][0]]
        buffer = buffers[p["buffer"]]
        count = sum(pieces[k]["rows"] * pieces[k]["cols"] for k, _ in slots[slot])
        if len(slots[slot]) == 1:
            ref = buffer.at[pl.ds(0, p["rows"]), pl.ds(0, p["cols"])]
        else:
            ref = buffer.at[pl.ds(0, count // buffer.shape[1])]
        return pltpu.make_async_remote_copy(
            src_ref=ref,
            dst_ref=ref,
            send_sem=sent.at[0],
            recv_sem=got.at[numbers[slot]],
            device_id={"rows": to["y", 1]},
            device_id_type=MESH,
        )

    def norm_copy(ref, n, axis, index):
        return pltpu.make_async_remote_copy(
            src_ref=ref,
            dst_ref=ref,
            send_sem=sent_norm.at[n],
            recv_sem=got_norm.at[n],
            device_id={axis: index},
            device_id_type=MESH,
        )

    def peer_copy(d):
        return norm_copy(peers.at[t], d - 1, "tp", ts[d])

    def y_copy(n):
        dy, link = ((0, ("y", 1)), (0, ("y", -1)), (NY - 1, ("y", 1)))[n]
        return norm_copy(norms.at[pl.ds(at[dy, 0], 1)], 3 + n, "rows", to[link])

    def z_copy(n):
        dz, link = (-n % NZ, ("z", 1)) if n < 4 else (n - 4, ("z", -1))
        return norm_copy(norms.at[pl.ds(zs[dz] * NY, NY)], 6 + n, "rows", to[link])

    def norm_step_0():
        for d in range(1, n_tp):
            peer_copy(d).start()

    def norm_step_1():
        for d in range(1, n_tp):
            peer_copy(d).wait_recv()
        norms[rows] = sum(peers[d] for d in range(n_tp))

    def norm_step_2():
        y_copy(0).start()
        y_copy(1).start()

    def norm_step_3():
        y_copy(0).wait_recv()
        y_copy(2).start()
        y_copy(1).wait_recv()

    def norm_step_4():
        y_copy(2).wait_recv()
        z_copy(0).start()
        z_copy(4).start()

    def norm_hop(n):
        z_copy(n - 1).wait_recv()
        z_copy(n).start()
        if n < 3:
            z_copy(n + 3).wait_recv()
            z_copy(n + 4).start()

    def norm_last():
        z_copy(3).wait_recv()
        z_copy(6).wait_recv()
        n_norm = norms.shape[0] * share * n_tp
        lane = lax.broadcasted_iota(jnp.int32, (1, 128), 1)
        lines = [jnp.zeros((1, 128), jnp.float32) for _ in range(n_norm // 128)]
        width = share * n_tp
        for r in range(norms.shape[0]):
            line, off = divmod(r * width, 128)
            part = pltpu.roll(norms[r], off, 1) if off else norms[r]
            lines[line] += jnp.where(lane >= off, part, 0.0)
            if off + width > 128:
                lines[line + 1] += jnp.where(lane < off + width - 128, part, 0.0)
        norm_out[...] = jnp.concatenate(lines, axis=0).astype(norm_out.dtype)

    def turn(j):
        part = mixed[128 * j : 128 * (j + 1), :]
        mixed_out[:, 128 * j : 128 * (j + 1)] = part.T

    turned = [s[0] for s in steps if s[1:3] == ("wait", ("last", 0))][0]
    end = steps[-1][0]
    n_turn = mixed.shape[0] // 128
    side_jobs = [(0.5, norm_step_0), (6.0, norm_step_1), (8.0, norm_step_2), (14.0, norm_step_3)]
    side_jobs += [(20.0, norm_step_4)]
    side_jobs += [(20.0 + 6.0 * n, functools.partial(norm_hop, n)) for n in range(1, 4)]
    side_jobs += [(46.0, norm_last)]
    gap = (end - 8.0 - turned) / n_turn
    side_jobs += [
        (turned + 0.01 + gap * j, functools.partial(turn, j)) for j in range(n_turn)
    ]
    side_jobs += [(min(s[0] for s in steps if s[1] == "send" and pieces[s[2]]["phase"]) - 0.01, merge_rest)]
    side_jobs.sort(key=lambda job: job[0])

    first = [s[0] >= HOLD or s[1] == "wait" for s in steps].index(True)
    down = ("z", -1)
    held = [copy(*s[2:5]) for s in steps[:first] if s[4] == down]

    def begin_down():
        pl.semaphore_wait(late, 1)
        for c in held:
            c.start()

    conditional = []
    for n, (when, what, piece, origin, link, detour) in enumerate(steps):
        while side_jobs and side_jobs[0][0] < when:
            side_jobs.pop(0)[1]()
        if n == first:
            pl.when(first_z)(begin_down)
        if what == "wait":
            arrival(piece).wait_recv()
        elif n < first and link == down:
            pl.when(jnp.logical_not(first_z))(copy(piece, origin, link).start)
        elif detour is None:
            copy(piece, origin, link).start()
        else:
            own = zs[origin[1]]
            hit = own == DETOURED if detour else own != DETOURED
            some = copy(piece, origin, link, len(conditional))
            pl.when(hit)(some.start)
            conditional.append((hit, some))
    for _, job in side_jobs:
        job()

    for hit, some in conditional:
        pl.when(hit)(some.wait_send)
    for phase, buffer in ((0, mixed), (1, rest)):
        other = buffer.shape[0] - depth
        for p in pieces:
            if p["phase"] == phase and p["detour"]:
                other -= len(p["detour"]) * p["rows"] * p["cols"] // buffer.shape[1]
        area = buffer.at[pl.ds(0, other)]
        pltpu.make_async_remote_copy(
            src_ref=area,
            dst_ref=area,
            send_sem=sent.at[phase],
            recv_sem=got.at[0],
            device_id={"rows": to["y", 1]},
            device_id_type=MESH,
        ).wait_send()
    for d in range(1, n_tp):
        peer_copy(d).wait_send()
    for n in range(3):
        y_copy(n).wait_send()
    for n in range(7):
        z_copy(n).wait_send()


def put_kernel(rest, mixed, norm, final_query, final_key, final_value, final_mixed, serve_norm, sems):
    q, k = final_query.shape[1], final_key.shape[1]
    moves = [(norm, serve_norm)]
    for source, final, cuts in (
        (mixed, final_mixed, 4),
        (rest.at[:, pl.ds(0, q)], final_query, 4),
        (rest.at[:, pl.ds(q, k)], final_key, 2),
        (rest.at[:, pl.ds(q + k, k)], final_value, 2),
    ):
        count = final.shape[0] // cuts
        for c in range(cuts):
            part = pl.ds(c * count, count)
            moves.append((source.at[part], final.at[part]))
    copies = [pltpu.make_async_copy(a, b, sems.at[n]) for n, (a, b) in enumerate(moves)]
    for c in copies:
        c.start()
    for c in copies:
        c.wait()


def shards(n_rows, n_tp, *args):
    (
        w_query,
        low_query,
        high_query,
        w_key,
        low_key,
        high_key,
        w_value,
        low_value,
        high_value,
        w_mixed,
        low_mixed,
        high_mixed,
        norm_train,
        norm_step,
    ) = args
    depth, q, k = w_query.shape[0], w_query.shape[1], w_key.shape[1]
    m = w_mixed.shape[0]
    total = n_rows * depth
    n_norm = n_rows * n_tp * norm_train.shape[0]
    bf16, f32 = jnp.bfloat16, jnp.float32
    vmem = pl.BlockSpec(memory_space=pltpu.VMEM)
    n_slots = len(plan(make_pieces(depth, m, q + 2 * k))[1])
    hbm = pl.BlockSpec(memory_space=pltpu.HBM)
    given = (
        w_query,
        low_query.T,
        high_query,
        w_key,
        low_key.T,
        high_key,
        w_value,
        low_value.T,
        high_value,
        w_mixed.T,
        low_mixed.T,
        high_mixed,
        norm_train.reshape(1, -1),
        norm_step.reshape(1, -1),
    )
    made = pl.pallas_call(
        functools.partial(gather_kernel, n_tp, depth),
        out_shape=(
            pltpu.VMEM((total, q + 2 * k), bf16),
            pltpu.VMEM((m, total), bf16),
            pltpu.VMEM((n_norm // 128, 128), bf16),
        ),
        in_specs=[hbm] * N_ARGS,
        out_specs=(vmem, vmem, vmem),
        scratch_shapes=[
            *(pltpu.VMEM(a.shape, a.dtype) for a in given),
            pltpu.VMEM((total, m), bf16),
            pltpu.VMEM((n_tp, 1, 128), f32),
            pltpu.VMEM((n_rows, 1, 128), f32),
            pltpu.SemaphoreType.DMA((N_ARGS,)),
            pltpu.SemaphoreType.REGULAR,
            pltpu.SemaphoreType.DMA((2,)),
            pltpu.SemaphoreType.DMA((2 * sum(len(d) for d in DETOUR.values()),)),
            pltpu.SemaphoreType.DMA((n_slots,)),
            pltpu.SemaphoreType.DMA((13,)),
            pltpu.SemaphoreType.DMA((13,)),
        ],
        compiler_params=pltpu.CompilerParams(
            collective_id=0, has_side_effects=True, vmem_limit_bytes=16 << 20
        ),
        name="gather",
    )(*(pltpu.with_memory_space_constraint(a, pltpu.HBM) for a in given))
    final_query, final_key, final_value, final_mixed, serve_norm = pl.pallas_call(
        put_kernel,
        out_shape=(
            jax.ShapeDtypeStruct((total, q), bf16),
            jax.ShapeDtypeStruct((total, k), bf16),
            jax.ShapeDtypeStruct((total, k), bf16),
            jax.ShapeDtypeStruct((m, total), bf16),
            jax.ShapeDtypeStruct((n_norm // 128, 128), bf16),
        ),
        in_specs=[vmem] * 3,
        out_specs=(hbm,) * 5,
        scratch_shapes=[pltpu.SemaphoreType.DMA((13,))],
        compiler_params=pltpu.CompilerParams(vmem_limit_bytes=2 << 20),
        name="put",
    )(*(pltpu.with_memory_space_constraint(a, pltpu.VMEM) for a in made))
    return final_query, final_key, final_value, final_mixed, serve_norm.reshape(-1)


def solution(mesh):
    return jax.shard_map(
        functools.partial(shards, mesh.shape["rows"], mesh.shape["tp"]),
        mesh=mesh,
        in_specs=(
            P(UNIT_ROWS, "tp"),
            P(UNIT_ROWS, None),
            P("unit", "tp"),
            P(UNIT_ROWS, "tp"),
            P(UNIT_ROWS, None),
            P("unit", "tp"),
            P(UNIT_ROWS, "tp"),
            P(UNIT_ROWS, None),
            P("unit", "tp"),
            P(("unit", "tp"), "rows"),
            P(("unit", "tp"), None),
            P("unit", "rows"),
            P(UNIT_ROWS_TP),
            P(UNIT_ROWS_TP),
        ),
        out_specs=(
            P("unit", "tp"),
            P("unit", "tp"),
            P("unit", "tp"),
            P(("unit", "tp"), None),
            P("unit"),
        ),
        check_vma=False,
    )
```

```python
import functools
import heapq

import jax
import jax.numpy as jnp
from jax import lax
from jax.experimental import pallas as pl
from jax.experimental.pallas import tpu as pltpu
from jax.sharding import PartitionSpec as P

MESH = pl.DeviceIdType.MESH
UNIT_ROWS = ("unit", "rows")
UNIT_ROWS_TP = ("unit", "rows", "tp")

mix_rate = 0.5
N_ARGS = 14

NY, NZ = 4, 8
SIZE = {"y": NY, "z": NZ}
LINKS = (("y", 1), ("y", -1), ("z", 1), ("z", -1))
RATE, LATENCY, LEAD = 46.6e3, 6.5, 7.5


DETOUR = {("rest", True, 0): (0, 1)}
DETOURED = NZ // 2
PAIRS = True
HOLD = 5.0


def reach(n, step, side):
    return n // 2 if (side == 0) == (step > 0) else n - 1 - n // 2


def onward(piece, via, hops):
    first, second = ("y", "z") if piece["y_first"] else ("z", "y")
    if via is None:
        out = [((axis, step), 1) for axis in (first, second) for step in (1, -1)]
    else:
        out = [(via, hops + 1)]
        if via[0] == first:
            out += [((second, step), 1) for step in (1, -1)]
    return [(l, h) for l, h in out if h <= reach(SIZE[l[0]], l[1], piece["side"])]


def slot_of(pieces, k, origin):
    piece, (dy, dz) = pieces[k], origin
    detoured = dy in piece["detour"] and dz == (NZ // 2 - 1 if piece["side"] == 0 else NZ // 2 + 1)
    if not onward(piece, *way_of(piece, origin)) and not detoured:
        return "last", piece["phase"]
    if PAIRS and piece["y_first"] and dz in (1, 2, NZ - 2, NZ - 1):
        return k - k % 2, (dy - dy % 2, dz)
    return k, origin


def way_of(piece, origin):
    dy, dz = origin
    axis = "z" if dz and (piece["y_first"] or not dy) else "y"
    n, off = SIZE[axis], dz if axis == "z" else dy
    if n - off <= reach(n, 1, piece["side"]):
        return (axis, 1), n - off
    return (axis, -1), off


def plan(pieces):
    def urgency(piece, link, hops):
        left = reach(SIZE[link[0]], link[1], piece["side"]) - hops
        first, second = ("y", "z") if piece["y_first"] else ("z", "y")
        return piece["phase"], -(left + (SIZE[second] // 2 if link[0] == first else 0))

    queue, free, seq = {l: [] for l in LINKS}, dict.fromkeys(LINKS, 0.0), 0
    events, steps, got, ready, last = [], [], {}, {}, dict.fromkeys(LINKS, 0.0)
    everywhere = [(k, (dy, dz)) for k in range(len(pieces)) for dy in range(NY) for dz in range(NZ) if dy or dz]
    slots = {}
    for k, origin in everywhere:
        slots.setdefault(slot_of(pieces, k, origin), []).append((k, origin))

    def hold(k, origin, via, hops):
        nonlocal seq
        for link, h in onward(pieces[k], via, hops):
            seq += 1
            heapq.heappush(queue[link], (urgency(pieces[k], link, h), seq, k, origin, h))

    for k in range(len(pieces)):
        ready[k, (0, 0)] = 0.0
        hold(k, (0, 0), None, 0)
    now = 0.0
    while True:
        for link in LINKS:
            if free[link] <= now + 1e-9 and queue[link]:
                _, _, k, origin, h = heapq.heappop(queue[link])
                issue = max(ready[k, origin], now - LEAD, last[link])
                last[link] = issue
                seq += 1
                steps.append((issue, seq, "send", k, origin, link))
                free[link] = now + pieces[k]["bytes"] / RATE
                heapq.heappush(events, (free[link], seq, None))
                heapq.heappush(events, (free[link] + LATENCY, seq, (k, beyond(origin, link), link, h)))
        if not events:
            break
        now = events[0][0]
        while events and events[0][0] <= now + 1e-9:
            _, _, landed = heapq.heappop(events)
            if landed is not None:
                k, origin, link, h = landed
                got[k, origin] = link, h
                slot = slot_of(pieces, k, origin)
                if all(one in got for one in slots[slot]):
                    seq += 1
                    steps.append((now, seq, "wait", slot, None, None))
                    for one in slots[slot]:
                        hold(*one, *got[one])
                        ready[one] = now
    steps.sort(key=lambda s: (s[0], s[2] == "send", s[1]))
    return [(t, *rest) for t, _, *rest in steps], slots


def beyond(origin, link):
    (dy, dz), (axis, step) = origin, link
    return ((dy - step) % NY, dz) if axis == "y" else (dy, (dz - step) % NZ)


def with_detours(steps, pieces, slots):
    steps = [(*s, None) for s in steps]
    for k, piece in enumerate(pieces):
        step = 1 if piece["side"] == 0 else -1
        near, far = step * (NZ // 2 - 1) % NZ, -step * (NZ // 2 - 1) % NZ
        for dy in piece["detour"]:
            what = [s[1:5] for s in steps]
            usual = what.index(("send", k, (dy, far), ("z", step)))
            slot = slot_of(pieces, k, (dy, near))
            at = max(usual, [w[:2] for w in what].index(("wait", slot)))
            steps[usual] = (*steps[usual][:5], False)
            steps.insert(at + 1, (steps[at][0], "send", k, (dy, near), ("z", -step), True))
    return steps


def make_pieces(depth, mixed, rest):
    pieces = []
    for phase, buffer, columns in ((0, "mixed", mixed), (1, "rest", rest)):
        cut = depth * 2 // 5 // 16 * 16
        for y_first, low, count in ((True, 0, cut), (False, cut, depth - cut)):
            for side in (0, 1):
                pieces.append(
                    dict(
                        phase=phase,
                        buffer=buffer,
                        y_first=y_first,
                        side=side,
                        row=low,
                        rows=count,
                        col=side * columns // 2,
                        cols=columns // 2,
                        bytes=count * columns,
                        detour=DETOUR.get((buffer, y_first, side), ()),
                    )
                )
    return pieces


def merged(w, low_t, high):
    product = lax.dot_general(
        low_t, high, (((0,), (0,)), ((), ())), preferred_element_type=jnp.float32
    )
    return (w.astype(jnp.float32) + mix_rate * product).astype(jnp.bfloat16)


def gather_kernel(n_tp, depth, *refs):
    given, (rest, mixed_out, norm_out), held = refs[:N_ARGS], refs[N_ARGS : N_ARGS + 3], refs[N_ARGS + 3 :]
    fetched, (mixed, peers, norms, fetch_sem, late, sent, sent_some, got, sent_norm, got_norm) = (
        held[:N_ARGS],
        held[N_ARGS:],
    )
    w_query, low_query, high_query, w_key, low_key, high_key, w_value, low_value, high_value = fetched[:9]
    w_mixed, low_mixed, high_mixed, norm_train, norm_step = fetched[9:]
    fetches = [
        pltpu.make_async_copy(a, b, fetch_sem.at[n])
        for n, (a, b) in enumerate(zip(given, fetched))
    ]
    for n in (*range(9, N_ARGS), *range(9)):
        fetches[n].start()

    rows, t = lax.axis_index("rows"), lax.axis_index("tp")
    z, y = rows // NY, lax.rem(rows, NY)
    ys = [lax.rem(y + d, NY) for d in range(NY)]
    zs = [lax.rem(z + d, NZ) for d in range(NZ)]
    ts = [lax.rem(t + d, n_tp) for d in range(n_tp)]
    at = {(dy, dz): zs[dz] * NY + ys[dy] for dy in range(NY) for dz in range(NZ)}
    to = {
        ("y", 1): at[1, 0],
        ("y", -1): at[NY - 1, 0],
        ("z", 1): at[0, 1],
        ("z", -1): at[0, NZ - 1],
    }

    barrier = pltpu.get_barrier_semaphore()
    first_z, last_z = z == 0, z == NZ - 1

    def greet(link, semaphore=barrier):
        pl.semaphore_signal(semaphore, 1, device_id={"rows": to[link]}, device_id_type=MESH)

    for link in LINKS:
        if link == ("z", 1):
            pl.when(jnp.logical_not(last_z))(functools.partial(greet, link))
        else:
            greet(link)
    for d in range(1, n_tp):
        pl.semaphore_signal(barrier, 1, device_id={"tp": ts[d]}, device_id_type=MESH)

    mine = pl.ds(pl.multiple_of(rows * depth, 16), depth)
    q, k = w_query.shape[1], w_key.shape[1]
    for n in range(9, N_ARGS):
        fetches[n].wait()
    mixed[mine, :] = merged(w_mixed[...], high_mixed[...], low_mixed[...])
    share = norm_train.shape[1]
    gain = norm_train[...] + norm_step[...]
    wide = jnp.concatenate([gain, jnp.zeros((1, 128 - share), jnp.float32)], axis=1)
    peers[t] = pltpu.roll(wide, t * share, 1)

    def merge_rest():
        for n in range(9):
            fetches[n].wait()
        rest[mine, :q] = merged(w_query[...], low_query[...], high_query[...])
        rest[mine, q : q + k] = merged(w_key[...], low_key[...], high_key[...])
        rest[mine, q + k :] = merged(w_value[...], low_value[...], high_value[...])

    pl.semaphore_wait(barrier, len(LINKS) + n_tp - 1 - first_z.astype(jnp.int32))
    pl.when(last_z)(functools.partial(greet, ("z", 1), late))

    buffers = {"mixed": mixed, "rest": rest}
    pieces = make_pieces(depth, mixed.shape[1], rest.shape[1])

    steps, slots = plan(pieces)
    steps = with_detours(steps, pieces, slots)
    numbers = {slot: n for n, slot in enumerate(slots)}

    def copy(k, origin, link, sent_by=None):
        p, r = pieces[k], at[origin]
        ref = buffers[p["buffer"]].at[
            pl.ds(pl.multiple_of(r * depth + p["row"], 16), p["rows"]),
            pl.ds(p["col"], p["cols"]),
        ]
        return pltpu.make_async_remote_copy(
            src_ref=ref,
            dst_ref=ref,
            send_sem=sent.at[p["phase"]] if sent_by is None else sent_some.at[sent_by],
            recv_sem=got.at[numbers[slot_of(pieces, k, beyond(origin, link))]],
            device_id={"rows": to[link]},
            device_id_type=MESH,
        )

    def arrival(slot):
        p = pieces[slots[slot][0][0]]
        buffer = buffers[p["buffer"]]
        count = sum(pieces[k]["rows"] * pieces[k]["cols"] for k, _ in slots[slot])
        if len(slots[slot]) == 1:
            ref = buffer.at[pl.ds(0, p["rows"]), pl.ds(0, p["cols"])]
        else:
            ref = buffer.at[pl.ds(0, count // buffer.shape[1])]
        return pltpu.make_async_remote_copy(
            src_ref=ref,
            dst_ref=ref,
            send_sem=sent.at[0],
            recv_sem=got.at[numbers[slot]],
            device_id={"rows": to["y", 1]},
            device_id_type=MESH,
        )

    def norm_copy(ref, n, axis, index):
        return pltpu.make_async_remote_copy(
            src_ref=ref,
            dst_ref=ref,
            send_sem=sent_norm.at[n],
            recv_sem=got_norm.at[n],
            device_id={axis: index},
            device_id_type=MESH,
        )

    def peer_copy(d):
        return norm_copy(peers.at[t], d - 1, "tp", ts[d])

    def y_copy(n):
        dy, link = ((0, ("y", 1)), (0, ("y", -1)), (NY - 1, ("y", 1)))[n]
        return norm_copy(norms.at[pl.ds(at[dy, 0], 1)], 3 + n, "rows", to[link])

    def z_copy(n):
        dz, link = (-n % NZ, ("z", 1)) if n < 4 else (n - 4, ("z", -1))
        return norm_copy(norms.at[pl.ds(zs[dz] * NY, NY)], 6 + n, "rows", to[link])

    def norm_step_0():
        for d in range(1, n_tp):
            peer_copy(d).start()

    def norm_step_1():
        for d in range(1, n_tp):
            peer_copy(d).wait_recv()
        norms[rows] = sum(peers[d] for d in range(n_tp))

    def norm_step_2():
        y_copy(0).start()
        y_copy(1).start()

    def norm_step_3():
        y_copy(0).wait_recv()
        y_copy(2).start()
        y_copy(1).wait_recv()

    def norm_step_4():
        y_copy(2).wait_recv()
        z_copy(0).start()
        z_copy(4).start()

    def norm_hop(n):
        z_copy(n - 1).wait_recv()
        z_copy(n).start()
        if n < 3:
            z_copy(n + 3).wait_recv()
            z_copy(n + 4).start()

    def norm_last():
        z_copy(3).wait_recv()
        z_copy(6).wait_recv()
        n_norm = norms.shape[0] * share * n_tp
        lane = lax.broadcasted_iota(jnp.int32, (1, 128), 1)
        lines = [jnp.zeros((1, 128), jnp.float32) for _ in range(n_norm // 128)]
        width = share * n_tp
        for r in range(norms.shape[0]):
            line, off = divmod(r * width, 128)
            part = pltpu.roll(norms[r], off, 1) if off else norms[r]
            lines[line] += jnp.where(lane >= off, part, 0.0)
            if off + width > 128:
                lines[line + 1] += jnp.where(lane < off + width - 128, part, 0.0)
        norm_out[...] = jnp.concatenate(lines, axis=0).astype(norm_out.dtype)

    def turn(j):
        part = mixed[128 * j : 128 * (j + 1), :]
        mixed_out[:, 128 * j : 128 * (j + 1)] = part.T

    turned = [s[0] for s in steps if s[1:3] == ("wait", ("last", 0))][0]
    end = steps[-1][0]
    n_turn = mixed.shape[0] // 128
    side_jobs = [(0.5, norm_step_0), (6.0, norm_step_1), (8.0, norm_step_2), (14.0, norm_step_3)]
    side_jobs += [(20.0, norm_step_4)]
    side_jobs += [(20.0 + 6.0 * n, functools.partial(norm_hop, n)) for n in range(1, 4)]
    side_jobs += [(46.0, norm_last)]
    gap = (end - 8.0 - turned) / n_turn
    side_jobs += [
        (turned + 0.01 + gap * j, functools.partial(turn, j)) for j in range(n_turn)
    ]
    side_jobs += [(min(s[0] for s in steps if s[1] == "send" and pieces[s[2]]["phase"]) - 0.01, merge_rest)]
    side_jobs.sort(key=lambda job: job[0])

    first = [s[0] >= HOLD or s[1] == "wait" for s in steps].index(True)
    down = ("z", -1)
    held = [copy(*s[2:5]) for s in steps[:first] if s[4] == down]

    def begin_down():
        pl.semaphore_wait(late, 1)
        for c in held:
            c.start()

    conditional = []
    for n, (when, what, piece, origin, link, detour) in enumerate(steps):
        while side_jobs and side_jobs[0][0] < when:
            side_jobs.pop(0)[1]()
        if n == first:
            pl.when(first_z)(begin_down)
        if what == "wait":
            arrival(piece).wait_recv()
        elif n < first and link == down:
            pl.when(jnp.logical_not(first_z))(copy(piece, origin, link).start)
        elif detour is None:
            copy(piece, origin, link).start()
        else:
            own = zs[origin[1]]
            hit = own == DETOURED if detour else own != DETOURED
            some = copy(piece, origin, link, len(conditional))
            pl.when(hit)(some.start)
            conditional.append((hit, some))
    for _, job in side_jobs:
        job()

    for hit, some in conditional:
        pl.when(hit)(some.wait_send)
    for phase, buffer in ((0, mixed), (1, rest)):
        other = buffer.shape[0] - depth
        for p in pieces:
            if p["phase"] == phase and p["detour"]:
                other -= len(p["detour"]) * p["rows"] * p["cols"] // buffer.shape[1]
        area = buffer.at[pl.ds(0, other)]
        pltpu.make_async_remote_copy(
            src_ref=area,
            dst_ref=area,
            send_sem=sent.at[phase],
            recv_sem=got.at[0],
            device_id={"rows": to["y", 1]},
            device_id_type=MESH,
        ).wait_send()
    for d in range(1, n_tp):
        peer_copy(d).wait_send()
    for n in range(3):
        y_copy(n).wait_send()
    for n in range(7):
        z_copy(n).wait_send()


def put_kernel(rest, mixed, norm, final_query, final_key, final_value, final_mixed, serve_norm, sems):
    q, k = final_query.shape[1], final_key.shape[1]
    moves = [
        (mixed, final_mixed),
        (rest.at[:, pl.ds(0, q)], final_query),
        (rest.at[:, pl.ds(q, k)], final_key),
        (rest.at[:, pl.ds(q + k, k)], final_value),
        (norm, serve_norm),
    ]
    copies = [pltpu.make_async_copy(a, b, sems.at[n]) for n, (a, b) in enumerate(moves)]
    for c in copies:
        c.start()
    for c in copies:
        c.wait()


def shards(n_rows, n_tp, *args):
    (
        w_query,
        low_query,
        high_query,
        w_key,
        low_key,
        high_key,
        w_value,
        low_value,
        high_value,
        w_mixed,
        low_mixed,
        high_mixed,
        norm_train,
        norm_step,
    ) = args
    depth, q, k = w_query.shape[0], w_query.shape[1], w_key.shape[1]
    m = w_mixed.shape[0]
    total = n_rows * depth
    n_norm = n_rows * n_tp * norm_train.shape[0]
    bf16, f32 = jnp.bfloat16, jnp.float32
    vmem = pl.BlockSpec(memory_space=pltpu.VMEM)
    n_slots = len(plan(make_pieces(depth, m, q + 2 * k))[1])
    hbm = pl.BlockSpec(memory_space=pltpu.HBM)
    given = (
        w_query,
        low_query.T,
        high_query,
        w_key,
        low_key.T,
        high_key,
        w_value,
        low_value.T,
        high_value,
        w_mixed.T,
        low_mixed.T,
        high_mixed,
        norm_train.reshape(1, -1),
        norm_step.reshape(1, -1),
    )
    made = pl.pallas_call(
        functools.partial(gather_kernel, n_tp, depth),
        out_shape=(
            pltpu.VMEM((total, q + 2 * k), bf16),
            pltpu.VMEM((m, total), bf16),
            pltpu.VMEM((n_norm // 128, 128), bf16),
        ),
        in_specs=[hbm] * N_ARGS,
        out_specs=(vmem, vmem, vmem),
        scratch_shapes=[
            *(pltpu.VMEM(a.shape, a.dtype) for a in given),
            pltpu.VMEM((total, m), bf16),
            pltpu.VMEM((n_tp, 1, 128), f32),
            pltpu.VMEM((n_rows, 1, 128), f32),
            pltpu.SemaphoreType.DMA((N_ARGS,)),
            pltpu.SemaphoreType.REGULAR,
            pltpu.SemaphoreType.DMA((2,)),
            pltpu.SemaphoreType.DMA((2 * sum(len(d) for d in DETOUR.values()),)),
            pltpu.SemaphoreType.DMA((n_slots,)),
            pltpu.SemaphoreType.DMA((13,)),
            pltpu.SemaphoreType.DMA((13,)),
        ],
        compiler_params=pltpu.CompilerParams(
            collective_id=0, has_side_effects=True, vmem_limit_bytes=16 << 20
        ),
        name="gather",
    )(*(pltpu.with_memory_space_constraint(a, pltpu.HBM) for a in given))
    final_query, final_key, final_value, final_mixed, serve_norm = pl.pallas_call(
        put_kernel,
        out_shape=(
            jax.ShapeDtypeStruct((total, q), bf16),
            jax.ShapeDtypeStruct((total, k), bf16),
            jax.ShapeDtypeStruct((total, k), bf16),
            jax.ShapeDtypeStruct((m, total), bf16),
            jax.ShapeDtypeStruct((n_norm // 128, 128), bf16),
        ),
        in_specs=[vmem] * 3,
        out_specs=(hbm,) * 5,
        scratch_shapes=[pltpu.SemaphoreType.DMA((5,))],
        compiler_params=pltpu.CompilerParams(vmem_limit_bytes=2 << 20),
        name="put",
    )(*(pltpu.with_memory_space_constraint(a, pltpu.VMEM) for a in made))
    return final_query, final_key, final_value, final_mixed, serve_norm.reshape(-1)


def solution(mesh):
    return jax.shard_map(
        functools.partial(shards, mesh.shape["rows"], mesh.shape["tp"]),
        mesh=mesh,
        in_specs=(
            P(UNIT_ROWS, "tp"),
            P(UNIT_ROWS, None),
            P("unit", "tp"),
            P(UNIT_ROWS, "tp"),
            P(UNIT_ROWS, None),
            P("unit", "tp"),
            P(UNIT_ROWS, "tp"),
            P(UNIT_ROWS, None),
            P("unit", "tp"),
            P(("unit", "tp"), "rows"),
            P(("unit", "tp"), None),
            P("unit", "rows"),
            P(UNIT_ROWS_TP),
            P(UNIT_ROWS_TP),
        ),
        out_specs=(
            P("unit", "tp"),
            P("unit", "tp"),
            P("unit", "tp"),
            P(("unit", "tp"), None),
            P("unit"),
        ),
        check_vma=False,
    )
```
